32 devices in a mesh: frame: 4 (over y, core), row: 8 (over z, x).
Axes of the slice: x: 2, y: 2, z: 4, core: 2. Of those that a mesh axis runs over, the one named last changes fastest.
Arguments:
- features: float32 [4, 32, 256, 256], P('frame', 'row'), may hold values from -6 to 6
- conv_weight: float32 [2, 3, 3, 256, 256], replicated, may hold values from -0.125 to 0.125
Outputs:
- activations: float32 [4, 32, 256, 256], P('frame', 'row')
The draws below stay inside these ranges and needn't reach their ends.
All inputs are finite; a program needn't handle non-finite values.
Results may differ from the reference program's by a relative error of at most 0.0001.
Values sent between devices are 32-bit elements; how exact they have to be, the bound alone decides.
A program may use at most 64 MiB of HBM per device.

```python
import jax
import jax.numpy as jnp
from jax import lax

C = 256
W = 256
LAYERS = 2
FRAMES = 4
H = 32


def block_levels(key, shape, shards, least, top_value):
    def one(position, shards_of):
        steps = jax.random.uniform(jax.random.fold_in(jax.random.fold_in(key, 6), position), (shards_of,), jnp.float32, least / len(shards), top_value / len(shards))
        return jnp.repeat(jnp.exp(steps), shape[position] // shards_of).reshape((-1,) + (1,) * (len(shape) - position - 1))

    factor_of = one(*shards[0])
    for cut in shards[1:]:
        factor_of = factor_of * one(*cut)
    return factor_of


def scatter_about(key, dims, deviation, reach, pieces=(), kind=jnp.bfloat16):
    factor_of = block_levels(key, dims, pieces, -0.22, 0.18) if pieces else 1.0
    result = jax.random.normal(key, dims, jnp.float32) * deviation * factor_of
    return jnp.minimum(jnp.maximum(result, -reach), reach).astype(kind)


def setup_inputs(seed: int = 0) -> dict:
    keys = jax.random.split(jax.random.key(seed), 3)
    features = scatter_about(keys[0], (FRAMES, H, W, C), 1.0, 6.0, ((0, 4), (1, 8)), jnp.float32)
    conv_weight = scatter_about(keys[1], (LAYERS, 3, 3, C, C), (9 * C) ** -0.5, 0.125, (), jnp.float32)
    return dict(features=features, conv_weight=conv_weight)


def temporal_shift(field):
    fold = field.shape[3] // 8
    zeros = jnp.zeros_like(field[:1, :, :, :fold])
    from_next = jnp.concatenate([field[1:, :, :, :fold], zeros], axis=0)
    from_prev = jnp.concatenate([zeros, field[:-1, :, :, fold:2 * fold]], axis=0)
    return jnp.concatenate([from_next, from_prev, field[:, :, :, 2 * fold:]], axis=3)


def convolve_frame(frame, kernel):
    rows, cols, chans = frame.shape
    padded = jnp.pad(frame, ((1, 1), (1, 1), (0, 0)))
    total = jnp.zeros((rows * cols, kernel.shape[3]), jnp.float32)
    for tap_row in range(3):
        for tap_col in range(3):
            window = padded[tap_row:tap_row + rows, tap_col:tap_col + cols, :].reshape(rows * cols, chans)
            total = total + jnp.dot(window, kernel[tap_row, tap_col], preferred_element_type=jnp.float32, precision=lax.Precision.HIGHEST)
    return jnp.maximum(total, 0.0).reshape(rows, cols, kernel.shape[3])


def reference(features, conv_weight):
    field = features
    for layer in range(LAYERS):
        shifted = temporal_shift(field)
        kernel = conv_weight[layer]
        field = lax.map(lambda frame: convolve_frame(frame, kernel), shifted)
    return field
```

```python
import jax
import jax.numpy as jnp
from jax import lax
from jax.experimental import pallas as pl
from jax.experimental.pallas import tpu as pltpu
from jax.sharding import PartitionSpec as P

MESH = pl.DeviceIdType.MESH
LANES = 128
PAD = 8
FAR, NEAR = 0, 1


def split(value):
    high = value.astype(jnp.bfloat16)
    low = (value - high.astype(jnp.float32)).astype(jnp.bfloat16)
    return high, low


def kernel(
    x_hbm, w_hbm, out, xin, wbuf, w3, sx, acc, mid, pack, got, half, hmain, hhalf, hshift,
    load_x, load_w, row_send, row_recv, frame_send, frame_recv,
):
    rows, cols, chans = xin.shape
    layers = wbuf.shape[0]
    fold = chans // 8
    last = rows - 1
    groups = LANES // fold
    part = cols // groups
    rest = LANES - 2 * fold
    halves = LANES // rest
    frames, bands = lax.axis_size("frame"), lax.axis_size("row")
    t, r = lax.axis_index("frame"), lax.axis_index("row")
    turned = r % 2
    sign = 1 - 2 * turned
    row_to = (r - sign, r + sign)
    has_row = tuple((peer >= 0) & (peer < bands) for peer in row_to)
    edge = (0, last)
    has_frame = (t > 0, t < frames - 1)
    frame_to = (t - 1, t + 1)

    def place(row, count):
        return row + turned * (count - 1 - 2 * row)

    loads_x = [pltpu.make_async_copy(x_hbm.at[0, place(q, rows)], xin.at[q], load_x.at[q]) for q in range(rows)]
    loads_w = [
        [pltpu.make_async_copy(w_hbm.at[n, place(d, 3)], wbuf.at[n, d], load_w.at[n, d]) for d in range(3)]
        for n in range(layers)
    ]
    for load in loads_x:
        load.start()
    for per_layer in loads_w:
        for load in per_layer:
            load.start()

    barrier = pltpu.get_barrier_semaphore()
    count = 0
    for have, axis, peers in ((has_row, "row", row_to), (has_frame, "frame", frame_to)):
        for side in range(2):
            count = count + have[side].astype(jnp.int32)

            @pl.when(have[side])
            def _():
                pl.semaphore_signal(barrier, inc=1, device_id={axis: peers[side]}, device_id_type=MESH)

    def maps(layer):
        return xin if layer == 0 else mid.at[layer - 1]

    def row_copy(layer, kind, piece):
        if piece == 0:
            source = maps(layer).at[edge[kind], :, pl.ds(LANES, chans - LANES)]
            target = hmain.at[layer, kind]
        elif piece == 1:
            source, target = half.at[layer, kind], hhalf.at[layer, kind]
        else:
            source = got.at[layer, piece - 2, edge[kind]]
            target = hshift.at[layer, kind, piece - 2]
        return pltpu.make_async_remote_copy(
            src_ref=source,
            dst_ref=target,
            send_sem=row_send.at[layer, kind, piece],
            recv_sem=row_recv.at[layer, kind, piece],
            device_id={"row": row_to[kind]},
            device_id_type=MESH,
        )

    def sent(kind, piece):
        return has_row[kind] if piece < 2 else has_row[kind] & has_frame[3 - piece]

    def each_piece(layer, kind, pieces, action):
        for piece in pieces:

            @pl.when(sent(kind, piece))
            def _():
                getattr(row_copy(layer, kind, piece), action)()

    def blocks(layer):
        return ((0, rows),) if layer == 0 else ((0, 1), (1, rows - 2), (last, 1))

    def frame_copy(layer, side, block):
        start, size = blocks(layer)[block]
        return pltpu.make_async_remote_copy(
            src_ref=pack.at[layer, side, pl.ds(start, size)],
            dst_ref=got.at[layer, side, pl.ds(start, size)],
            send_sem=frame_send.at[layer, side, block],
            recv_sem=frame_recv.at[layer, side, block],
            device_id={"frame": frame_to[side]},
            device_id_type=MESH,
        )

    def pack_frames(layer, block):
        start, size = blocks(layer)[block]
        lane = lax.broadcasted_iota(jnp.int32, (part, LANES), 1)
        for side in range(2):
            for row in range(start, start + size):
                full = None
                for group in range(groups):
                    value = maps(layer)[row, pl.ds(group * part, part), pl.ds(0, LANES)]
                    shift = ((group - side) * fold) % LANES
                    value = pltpu.roll(value, shift, 1) if shift else value
                    full = value if full is None else jnp.where(lane // fold == group, value, full)
                pack[layer, side, row] = full

    def send_frames(layer, block):
        for side in range(2):

            @pl.when(has_frame[side])
            def _():
                frame_copy(layer, side, block).start()

    def take_frames(layer, block):
        for side in range(2):

            @pl.when(has_frame[1 - side])
            def _():
                frame_copy(layer, side, block).wait_recv()

    def pack_half(layer, kind):
        size = cols // halves
        lane = lax.broadcasted_iota(jnp.int32, (size, LANES), 1)
        full = None
        for group in range(halves):
            value = maps(layer)[edge[kind], pl.ds(group * size, size), pl.ds(0, LANES)]
            shift = (group * rest - 2 * fold) % LANES
            value = pltpu.roll(value, shift, 1) if shift else value
            full = value if full is None else jnp.where(lane // rest == group, value, full)
        half[layer, kind] = full

    def put(spot, start, size, tile, value):
        high, low = split(value)
        sx[spot, pl.ds(start, size), pl.ds(tile, value.shape[1])] = high
        sx[spot, pl.ds(start, size), pl.ds(chans + tile, value.shape[1])] = low
        sx[spot, pl.ds(start, size), pl.ds(2 * chans + tile, value.shape[1])] = high

    def put_lower(spot, rest_of, shifted):
        lane = lax.broadcasted_iota(jnp.int32, (part, LANES), 1)
        for group in range(groups):
            value = rest_of(group * part)
            for side in range(2):
                moved = shifted(side)
                shift = ((side - group) * fold) % LANES
                moved = pltpu.roll(moved, shift, 1) if shift else moved
                value = jnp.where(lane // fold == side, moved, value)
            put(spot, group * part, part, 0, value)

    def put_row(layer, row):
        put_lower(
            row + 1,
            lambda start: maps(layer)[row, pl.ds(start, part), pl.ds(0, LANES)],
            lambda side: got[layer, side, row],
        )
        put(row + 1, 0, cols, LANES, maps(layer)[row, :, pl.ds(LANES, chans - LANES)])

    def put_halo(layer, kind):
        spot = 0 if kind == FAR else rows + 1
        size = cols // halves

        def rest_of(start):
            group = start // size
            value = hhalf[layer, kind, pl.ds(start - group * size, part)]
            shift = (2 * fold - group * rest) % LANES
            return pltpu.roll(value, shift, 1) if shift else value

        put_lower(spot, rest_of, lambda side: hshift[layer, kind, side])
        put(spot, 0, cols, LANES, hmain[layer, kind])

    def split_weights(layer):
        for load in loads_w[layer]:
            load.wait()

        def tap(index, carry):
            down, across = index // 3, index % 3
            high, low = split(wbuf[layer, down, across])
            base = pl.multiple_of(down * 3 * chans, 3 * chans)
            w3[layer, across, pl.ds(base, chans)] = high
            w3[layer, across, pl.ds(base + chans, chans)] = high
            w3[layer, across, pl.ds(base + 2 * chans, chans)] = low
            return carry

        lax.fori_loop(0, 9, tap, 0)

    def inner(layer, parts, first_tap, taps):
        def across(tap, carry):
            for first, count, low, high, add in parts:
                left = jnp.concatenate(
                    [
                        sx[pl.ds(first + down, count)].reshape(count * cols, 3 * chans)
                        for down in range(low, high)
                    ],
                    axis=1,
                )
                right = w3[layer, tap, pl.ds(low * 3 * chans, (high - low) * 3 * chans)]
                total = jnp.dot(left, right, preferred_element_type=jnp.float32)
                total = total.reshape(count, cols, chans)
                if add:
                    acc[tap, pl.ds(first, count), pl.ds(PAD, cols)] += total
                else:
                    acc[tap, pl.ds(first, count), pl.ds(PAD, cols)] = total
            return carry

        lax.fori_loop(first_tap, first_tap + taps, across, 0)

    whole_parts = ((0, 1, 1, 3, False), (1, rows - 2, 0, 3, False), (last, 1, 0, 2, False))
    early_parts = ((0, 1, 2, 3, False), (1, 1, 1, 3, False), (2, rows - 3, 0, 3, False), (last, 1, 0, 2, False))
    late_parts = ((0, 1, 1, 2, True), (1, 1, 0, 1, True))

    def outer(layer, kind):
        @pl.when(has_row[kind])
        def _():
            each_piece(layer, kind, range(4), "wait_recv")
            put_halo(layer, kind)

        inner(layer, ((0, 1, 0, 1, True),) if kind == FAR else ((last, 1, 2, 3, True),), 0, 3)

    def finish(layer, row):
        total = acc[0, row, pl.ds(PAD - 1, cols)] + acc[1, row, pl.ds(PAD, cols)]
        total = jnp.maximum(total + acc[2, row, pl.ds(PAD + 1, cols)], 0.0)
        if layer == layers - 1:
            out[place(row, rows)] = total
        else:
            mid[layer, row] = total

    def blank():
        acc[:, :, pl.ds(0, PAD)] = jnp.zeros((3, rows, PAD, chans), jnp.float32)
        acc[:, :, pl.ds(PAD + cols, PAD)] = jnp.zeros((3, rows, PAD, chans), jnp.float32)
        for kind, spot in ((FAR, 0), (NEAR, rows + 1)):

            @pl.when(jnp.logical_not(has_row[kind]))
            def _():
                sx[spot] = jnp.zeros((cols, 3 * chans), jnp.bfloat16)

        for side in range(2):

            @pl.when(jnp.logical_not(has_frame[1 - side]))
            def _():
                for layer in range(layers):
                    got[layer, side] = jnp.zeros((rows, part, LANES), jnp.float32)
                    for kind in range(2):
                        hshift[layer, kind, side] = jnp.zeros((part, LANES), jnp.float32)

    for load in loads_x:
        load.wait()
    pack_frames(0, 0)
    pack_half(0, NEAR)
    pack_half(0, FAR)
    blank()
    pl.semaphore_wait(barrier, count)
    send_frames(0, 0)
    each_piece(0, NEAR, range(2), "start")
    split_weights(0)
    take_frames(0, 0)
    each_piece(0, NEAR, range(2, 4), "start")
    for row in range(rows):
        put_row(0, row)
    inner(0, whole_parts, 0, 1)
    each_piece(0, FAR, range(4), "start")
    inner(0, whole_parts, 1, 2)
    for layer in range(layers):
        final = layer == layers - 1
        outer(layer, NEAR)
        finish(layer, last)
        if not final:
            each_piece(layer + 1, NEAR, range(1), "start")
            pack_frames(layer + 1, 2)
            send_frames(layer + 1, 2)
            pack_half(layer + 1, NEAR)
            each_piece(layer + 1, NEAR, range(1, 2), "start")
        for row in range(1, last):
            finish(layer, row)
        if not final:
            pack_frames(layer + 1, 1)
            send_frames(layer + 1, 1)
            split_weights(layer + 1)
            take_frames(layer + 1, 2)
            each_piece(layer + 1, NEAR, range(2, 4), "start")
            put_row(layer + 1, last)
            take_frames(layer + 1, 1)
            for row in range(1, last):
                put_row(layer + 1, row)
        outer(layer, FAR)
        finish(layer, 0)
        if not final:
            each_piece(layer + 1, FAR, range(1), "start")
            pack_frames(layer + 1, 0)
            send_frames(layer + 1, 0)
            pack_half(layer + 1, FAR)
            each_piece(layer + 1, FAR, range(1, 2), "start")
            inner(layer + 1, early_parts, 0, 1)
            take_frames(layer + 1, 0)
            each_piece(layer + 1, FAR, range(2, 4), "start")
            inner(layer + 1, early_parts, 1, 2)
            put_row(layer + 1, 0)
            inner(layer + 1, late_parts, 0, 3)

    for layer in range(layers):
        for kind in range(2):
            each_piece(layer, kind, range(4), "wait_send")
        for side in range(2):
            for block in range(len(blocks(layer))):

                @pl.when(has_frame[side])
                def _():
                    frame_copy(layer, side, block).wait_send()


def store(y_ref, o_hbm, sem):
    copies = [pltpu.make_async_copy(y_ref.at[n], o_hbm.at[0, n], sem.at[n]) for n in range(y_ref.shape[0])]
    for copy in copies:
        copy.start()
    for copy in copies:
        copy.wait()


def local(features, conv_weight):
    _, rows, cols, chans = features.shape
    layers = conv_weight.shape[0]
    fold = chans // 8
    part = cols // (LANES // fold)
    halved = cols // (LANES // (LANES - 2 * fold))
    f32, bf16 = jnp.float32, jnp.bfloat16
    dma = pltpu.SemaphoreType.DMA
    result = pl.pallas_call(
        kernel,
        out_shape=pltpu.VMEM((rows, cols, chans), f32),
        in_specs=[pl.BlockSpec(memory_space=pl.ANY)] * 2,
        out_specs=pl.BlockSpec(memory_space=pltpu.VMEM),
        scratch_shapes=[
            pltpu.VMEM((rows, cols, chans), f32),
            pltpu.VMEM(conv_weight.shape, f32),
            pltpu.VMEM((layers, 3, 9 * chans, chans), bf16),
            pltpu.VMEM((rows + 2, cols, 3 * chans), bf16),
            pltpu.VMEM((3, rows, cols + 2 * PAD, chans), f32),
            pltpu.VMEM((layers - 1, rows, cols, chans), f32),
            pltpu.VMEM((layers, 2, rows, part, LANES), f32),
            pltpu.VMEM((layers, 2, rows, part, LANES), f32),
            pltpu.VMEM((layers, 2, halved, LANES), f32),
            pltpu.VMEM((layers, 2, cols, chans - LANES), f32),
            pltpu.VMEM((layers, 2, halved, LANES), f32),
            pltpu.VMEM((layers, 2, 2, part, LANES), f32),
            dma((rows,)),
            dma((layers, 3)),
            dma((layers, 2, 4)),
            dma((layers, 2, 4)),
            dma((layers, 2, 3)),
            dma((layers, 2, 3)),
        ],
        compiler_params=pltpu.CompilerParams(
            collective_id=0, has_side_effects=True, vmem_limit_bytes=62 * 1024 * 1024
        ),
    )(features, conv_weight)
    return pl.pallas_call(
        store,
        out_shape=jax.ShapeDtypeStruct(features.shape, f32),
        in_specs=[pl.BlockSpec(memory_space=pltpu.VMEM)],
        out_specs=pl.BlockSpec(memory_space=pl.ANY),
        scratch_shapes=[dma((rows,))],
        compiler_params=pltpu.CompilerParams(vmem_limit_bytes=2 * 1024 * 1024),
    )(result)


def solution(mesh):
    placed = (P("frame", "row", None, None), P())
    return jax.shard_map(
        local, mesh=mesh, in_specs=placed, out_specs=P("frame", "row", None, None), check_vma=False
    )
```

```python
import jax
import jax.numpy as jnp
from jax import lax
from jax.experimental import pallas as pl
from jax.experimental.pallas import tpu as pltpu
from jax.sharding import PartitionSpec as P

MESH = pl.DeviceIdType.MESH
LANES = 128
PAD = 8
FAR, NEAR = 0, 1


def split(value):
    high = value.astype(jnp.bfloat16)
    low = (value - high.astype(jnp.float32)).astype(jnp.bfloat16)
    return high, low


def kernel(
    x_hbm, w_hbm, out, xin, wbuf, w3, sx, acc, mid, pack, got, half, hmain, hhalf, hshift, rmain, rhalf,
    load_x, load_w, row_send, row_recv, frame_send, frame_recv, relay_send, relay_recv,
):
    rows, cols, chans = xin.shape
    layers = wbuf.shape[0]
    tiles = chans // LANES
    both = range(tiles)
    fold = chans // 8
    last = rows - 1
    groups = LANES // fold
    part = cols // groups
    rest = LANES - 2 * fold
    halves = LANES // rest
    frames, bands = lax.axis_size("frame"), lax.axis_size("row")
    t, r = lax.axis_index("frame"), lax.axis_index("row")
    turned = r % 2
    sign = 1 - 2 * turned
    row_to = (r - sign, r + sign)
    has_row = tuple((peer >= 0) & (peer < bands) for peer in row_to)
    edge = (0, last)
    has_frame = (t > 0, t < frames - 1)
    frame_to = (t - 1, t + 1)

    pairs = bands // 2

    def shared(place):
        step = place // 2
        return 4 * (step + (place % 2) * (pairs - 1 - 2 * step)) // pairs

    def takes(place, piece):
        quarters = shared(place)
        return quarters >= 2 if piece == 0 else quarters % 2 == 1

    def within(place):
        return (place >= 0) & (place < bands)

    def relayed(piece):
        return has_row[FAR] & has_row[NEAR] & takes(r, piece)

    onward = r + 2 * sign
    behind = r - 2 * sign

    def relays(piece):
        return has_row[NEAR] & within(onward) & takes(row_to[NEAR], piece)

    def place(row, count):
        return row + turned * (count - 1 - 2 * row)

    loads_x = [pltpu.make_async_copy(x_hbm.at[0, place(q, rows)], xin.at[q], load_x.at[q]) for q in range(rows)]
    loads_w = [
        [pltpu.make_async_copy(w_hbm.at[n, place(d, 3)], wbuf.at[n, d], load_w.at[n, d]) for d in range(3)]
        for n in range(layers)
    ]
    for load in loads_x:
        load.start()

    barrier = pltpu.get_barrier_semaphore()
    count = 0
    for have, axis, peers in ((has_row, "row", row_to), (has_frame, "frame", frame_to)):
        for side in range(2):
            count = count + have[side].astype(jnp.int32)

            @pl.when(have[side])
            def _():
                pl.semaphore_signal(barrier, inc=1, device_id={axis: peers[side]}, device_id_type=MESH)

    for peer in (onward, behind):
        count = count + within(peer).astype(jnp.int32)

        @pl.when(within(peer))
        def _():
            pl.semaphore_signal(barrier, inc=1, device_id={"row": peer}, device_id_type=MESH)

    def maps(layer):
        return xin if layer == 0 else mid.at[layer - 1]

    def row_copy(layer, kind, piece, relay=False):
        if piece == 0:
            upper = pl.ds(LANES, chans - LANES)
            if layer == 0:
                source = x_hbm.at[0, place(edge[kind], rows), :, upper]
            else:
                source = maps(layer).at[edge[kind], :, upper]
            target = hmain.at[layer, kind]
        elif piece == 1:
            source, target = half.at[layer, kind], hhalf.at[layer, kind]
        else:
            source = got.at[layer, piece - 2, edge[kind]]
            target = hshift.at[layer, kind, piece - 2]
        return pltpu.make_async_remote_copy(
            src_ref=source,
            dst_ref=(rmain, rhalf)[piece].at[layer] if relay else target,
            send_sem=row_send.at[layer, kind, piece],
            recv_sem=relay_recv.at[layer, piece] if relay else row_recv.at[layer, kind, piece],
            device_id={"row": row_to[NEAR if relay else kind]},
            device_id_type=MESH,
        )

    def relay_copy(layer, piece):
        return pltpu.make_async_remote_copy(
            src_ref=(rmain, rhalf)[piece].at[layer],
            dst_ref=(hmain, hhalf)[piece].at[layer, FAR],
            send_sem=relay_send.at[layer, piece],
            recv_sem=row_recv.at[layer, FAR, piece],
            device_id={"row": onward},
            device_id_type=MESH,
        )

    def start_far(layer, piece):
        @pl.when(relayed(piece))
        def _():
            row_copy(layer, FAR, piece, True).start()

        @pl.when(has_row[FAR] & jnp.logical_not(relayed(piece)))
        def _():
            row_copy(layer, FAR, piece).start()

    def forward(layer, piece):
        @pl.when(relays(piece))
        def _():
            row_copy(layer, FAR, piece, True).wait_recv()
            relay_copy(layer, piece).start()

    def sent(kind, piece):
        return has_row[kind] if piece < 2 else has_row[kind] & has_frame[3 - piece]

    def each_piece(layer, kind, pieces, action):
        for piece in pieces:

            @pl.when(sent(kind, piece))
            def _():
                getattr(row_copy(layer, kind, piece), action)()

    blocks = ((0, 1), (1, rows - 2), (last, 1))

    def frame_copy(layer, side, block):
        start, size = blocks[block]
        return pltpu.make_async_remote_copy(
            src_ref=pack.at[layer, side, pl.ds(start, size)],
            dst_ref=got.at[layer, side, pl.ds(start, size)],
            send_sem=frame_send.at[layer, side, block],
            recv_sem=frame_recv.at[layer, side, block],
            device_id={"frame": frame_to[side]},
            device_id_type=MESH,
        )

    def pack_frames(layer, block):
        start, size = blocks[block]
        lane = lax.broadcasted_iota(jnp.int32, (part, LANES), 1)
        for side in range(2):
            for row in range(start, start + size):
                full = None
                for group in range(groups):
                    value = maps(layer)[row, pl.ds(group * part, part), pl.ds(0, LANES)]
                    shift = ((group - side) * fold) % LANES
                    value = pltpu.roll(value, shift, 1) if shift else value
                    full = value if full is None else jnp.where(lane // fold == group, value, full)
                pack[layer, side, row] = full

    def send_frames(layer, block):
        for side in range(2):

            @pl.when(has_frame[side])
            def _():
                frame_copy(layer, side, block).start()

    def take_frames(layer, block):
        for side in range(2):

            @pl.when(has_frame[1 - side])
            def _():
                frame_copy(layer, side, block).wait_recv()

    def pack_half(layer, kind):
        size = cols // halves
        lane = lax.broadcasted_iota(jnp.int32, (size, LANES), 1)
        full = None
        for group in range(halves):
            value = maps(layer)[edge[kind], pl.ds(group * size, size), pl.ds(0, LANES)]
            shift = (group * rest - 2 * fold) % LANES
            value = pltpu.roll(value, shift, 1) if shift else value
            full = value if full is None else jnp.where(lane // rest == group, value, full)
        half[layer, kind] = full

    def put(spot, start, size, tile, value):
        high, low = split(value)
        for n, piece in enumerate((high, low, high)):
            sx[spot, pl.ds(start, size), pl.ds((3 * tile + n) * LANES, LANES)] = piece

    def put_upper(spot, source):
        for tile in range(1, tiles):
            put(spot, 0, cols, tile, source[:, pl.ds((tile - 1) * LANES, LANES)])

    def put_lower(spot, rest_of, shifted):
        lane = lax.broadcasted_iota(jnp.int32, (part, LANES), 1)
        for group in range(groups):
            value = rest_of(group * part)
            for side in range(2):
                moved = shifted(side)
                shift = ((side - group) * fold) % LANES
                moved = pltpu.roll(moved, shift, 1) if shift else moved
                value = jnp.where(lane // fold == side, moved, value)
            put(spot, group * part, part, 0, value)

    def put_row_upper(layer, row):
        put_upper(row + 1, maps(layer).at[row, :, pl.ds(LANES, chans - LANES)])

    def put_row_lower(layer, row):
        put_lower(
            row + 1,
            lambda start: maps(layer)[row, pl.ds(start, part), pl.ds(0, LANES)],
            lambda side: got[layer, side, row],
        )

    def put_halo(layer, kind):
        spot = 0 if kind == FAR else rows + 1
        size = cols // halves

        def rest_of(start):
            group = start // size
            value = hhalf[layer, kind, pl.ds(start - group * size, part)]
            shift = (2 * fold - group * rest) % LANES
            return pltpu.roll(value, shift, 1) if shift else value

        put_lower(spot, rest_of, lambda side: hshift[layer, kind, side])
        put_upper(spot, hmain.at[layer, kind])

    def split_weights(layer):
        for load in loads_w[layer]:
            load.wait()

        def tap(index, carry):
            down, across = index // 3, index % 3
            high, low = split(wbuf[layer, down, across])
            for tile in range(tiles):
                span = slice(tile * LANES, (tile + 1) * LANES)
                base = pl.multiple_of((3 * tile + down) * 3 * LANES, LANES)
                for n, piece in enumerate((high, high, low)):
                    w3[layer, across, pl.ds(base + n * LANES, LANES)] = piece[span]
            return carry

        lax.fori_loop(0, 9, tap, 0)

    def parts_of(sources, seen):
        parts = []
        for row in range(rows):
            downs = [down for down in range(3) if row + down - 1 in sources]
            if downs:
                key = (downs[0], downs[-1] + 1, row in seen)
                if parts and parts[-1][2:] == key and sum(parts[-1][:2]) == row:
                    parts[-1] = (parts[-1][0], parts[-1][1] + 1) + key
                else:
                    parts.append((row, 1) + key)
        seen.update(part[0] + n for part in parts for n in range(part[1]))
        return parts

    def inner(layer, parts, first_tap, taps, which):
        deep = 3 * LANES

        def across(tap, carry):
            for first, count, low, high, add in parts:
                left = jnp.concatenate(
                    [
                        sx[pl.ds(first + down, count), :, pl.ds(tile * deep, deep)].reshape(count * cols, deep)
                        for tile in which
                        for down in range(low, high)
                    ],
                    axis=1,
                )
                right = jnp.concatenate(
                    [
                        w3[layer, tap, pl.ds((3 * tile + low) * deep, (high - low) * deep)]
                        for tile in which
                    ],
                    axis=0,
                )
                total = jnp.dot(left, right, preferred_element_type=jnp.float32)
                total = total.reshape(count, cols, chans)
                if add:
                    acc[layer % 2, tap, pl.ds(first, count), pl.ds(PAD, cols)] += total
                else:
                    acc[layer % 2, tap, pl.ds(first, count), pl.ds(PAD, cols)] = total
            return carry

        lax.fori_loop(first_tap, first_tap + taps, across, 0)

    def outer(layer, kind):
        @pl.when(has_row[kind])
        def _():
            each_piece(layer, kind, range(4), "wait_recv")
            put_halo(layer, kind)

        inner(layer, ((0, 1, 0, 1, True),) if kind == FAR else ((last, 1, 2, 3, True),), 0, 3, both)

    def finish(layer, row):
        part = acc.at[layer % 2, :, row]
        total = part[0, pl.ds(PAD - 1, cols)] + part[1, pl.ds(PAD, cols)]
        total = jnp.maximum(total + part[2, pl.ds(PAD + 1, cols)], 0.0)
        if layer == layers - 1:
            out[place(row, rows)] = total
        else:
            mid[layer, row] = total

    def blank():
        margin = jnp.zeros((2, 3, rows, PAD, chans), jnp.float32)
        acc[:, :, :, pl.ds(0, PAD)] = margin
        acc[:, :, :, pl.ds(PAD + cols, PAD)] = margin
        for kind, spot in ((FAR, 0), (NEAR, rows + 1)):

            @pl.when(jnp.logical_not(has_row[kind]))
            def _():
                sx[spot] = jnp.zeros((cols, 3 * chans), jnp.bfloat16)

        for side in range(2):

            @pl.when(jnp.logical_not(has_frame[1 - side]))
            def _():
                for layer in range(layers):
                    got[layer, side] = jnp.zeros((rows, part, LANES), jnp.float32)
                    for kind in range(2):
                        hshift[layer, kind, side] = jnp.zeros((part, LANES), jnp.float32)

    pl.semaphore_wait(barrier, count)
    start_far(0, 0)
    for load in loads_x:
        load.wait()
    pack_half(0, FAR)
    start_far(0, 1)
    each_piece(0, NEAR, range(1), "start")
    for per_layer in loads_w:
        for load in per_layer:
            load.start()
    for block in (0, 2, 1):
        pack_frames(0, block)
        send_frames(0, block)
    pack_half(0, NEAR)
    each_piece(0, NEAR, range(1, 2), "start")
    blank()
    for row in range(rows):
        put_row_upper(0, row)
    split_weights(0)
    seen = set()
    parts = parts_of(range(rows), seen)
    inner(0, parts, 0, 1, both[1:])
    take_frames(0, 0)
    each_piece(0, FAR, range(2, 4), "start")
    take_frames(0, 2)
    each_piece(0, NEAR, range(2, 4), "start")
    inner(0, parts, 1, 2, both[1:])
    take_frames(0, 1)
    for row in range(rows):
        put_row_lower(0, row)
    parts = parts_of(range(rows), seen)
    forward(0, 0)
    inner(0, parts, 0, 2, both[:1])
    forward(0, 1)
    inner(0, parts, 2, 1, both[:1])
    for layer in range(layers):
        final = layer == layers - 1
        after = layer + 1
        for row in range(1, last):
            finish(layer, row)
        if not final:
            pack_frames(after, 1)
            send_frames(after, 1)
            split_weights(after)
        outer(layer, FAR)
        finish(layer, 0)
        if not final:
            start_far(after, 0)
            pack_half(after, FAR)
            start_far(after, 1)
            pack_frames(after, 0)
            send_frames(after, 0)
        outer(layer, NEAR)
        finish(layer, last)
        if not final:
            each_piece(after, NEAR, range(1), "start")
            pack_frames(after, 2)
            send_frames(after, 2)
            pack_half(after, NEAR)
            each_piece(after, NEAR, range(1, 2), "start")
            take_frames(after, 1)
            for row in range(1, last):
                put_row_upper(after, row)
                put_row_lower(after, row)
            seen = set()
            parts = parts_of(range(1, last), seen)
            inner(after, parts, 0, 2, both)
            take_frames(after, 0)
            each_piece(after, FAR, range(2, 4), "start")
            forward(after, 0)
            inner(after, parts, 2, 1, both)
            take_frames(after, 2)
            each_piece(after, NEAR, range(2, 4), "start")
            put_row_upper(after, 0)
            put_row_lower(after, 0)
            inner(after, parts_of((0,), seen), 0, 3, both)
            forward(after, 1)
            put_row_upper(after, last)
            put_row_lower(after, last)
            inner(after, parts_of((last,), seen), 0, 3, both)

    for layer in range(layers):
        for kind in range(2):
            each_piece(layer, kind, range(4), "wait_send")
        for piece in range(2):

            @pl.when(relays(piece))
            def _():
                relay_copy(layer, piece).wait_send()

        for side in range(2):
            for block in range(len(blocks)):

                @pl.when(has_frame[side])
                def _():
                    frame_copy(layer, side, block).wait_send()


def store(y_ref, o_hbm, sem):
    copies = [pltpu.make_async_copy(y_ref.at[n], o_hbm.at[0, n], sem.at[n]) for n in range(y_ref.shape[0])]
    for copy in copies:
        copy.start()
    for copy in copies:
        copy.wait()


def local(features, conv_weight):
    _, rows, cols, chans = features.shape
    layers = conv_weight.shape[0]
    fold = chans // 8
    part = cols // (LANES // fold)
    halved = cols // (LANES // (LANES - 2 * fold))
    f32, bf16 = jnp.float32, jnp.bfloat16
    dma = pltpu.SemaphoreType.DMA
    result = pl.pallas_call(
        kernel,
        out_shape=pltpu.VMEM((rows, cols, chans), f32),
        in_specs=[pl.BlockSpec(memory_space=pl.ANY)] * 2,
        out_specs=pl.BlockSpec(memory_space=pltpu.VMEM),
        scratch_shapes=[
            pltpu.VMEM((rows, cols, chans), f32),
            pltpu.VMEM(conv_weight.shape, f32),
            pltpu.VMEM((layers, 3, 9 * chans, chans), bf16),
            pltpu.VMEM((rows + 2, cols, 3 * chans), bf16),
            pltpu.VMEM((2, 3, rows, cols + 2 * PAD, chans), f32),
            pltpu.VMEM((layers - 1, rows, cols, chans), f32),
            pltpu.VMEM((layers, 2, rows, part, LANES), f32),
            pltpu.VMEM((layers, 2, rows, part, LANES), f32),
            pltpu.VMEM((layers, 2, halved, LANES), f32),
            pltpu.VMEM((layers, 2, cols, chans - LANES), f32),
            pltpu.VMEM((layers, 2, halved, LANES), f32),
            pltpu.VMEM((layers, 2, 2, part, LANES), f32),
            pltpu.VMEM((layers, cols, chans - LANES), f32),
            pltpu.VMEM((layers, halved, LANES), f32),
            dma((rows,)),
            dma((layers, 3)),
            dma((layers, 2, 4)),
            dma((layers, 2, 4)),
            dma((layers, 2, 3)),
            dma((layers, 2, 3)),
            dma((layers, 2)),
            dma((layers, 2)),
        ],
        compiler_params=pltpu.CompilerParams(
            collective_id=0, has_side_effects=True, vmem_limit_bytes=62 * 1024 * 1024
        ),
    )(features, conv_weight)
    return pl.pallas_call(
        store,
        out_shape=jax.ShapeDtypeStruct(features.shape, f32),
        in_specs=[pl.BlockSpec(memory_space=pltpu.VMEM)],
        out_specs=pl.BlockSpec(memory_space=pl.ANY),
        scratch_shapes=[dma((rows,))],
        compiler_params=pltpu.CompilerParams(vmem_limit_bytes=2 * 1024 * 1024),
    )(result)


def solution(mesh):
    placed = (P("frame", "row", None, None), P())
    return jax.shard_map(
        local, mesh=mesh, in_specs=placed, out_specs=P("frame", "row", None, None), check_vma=False
    )
```

```python
import jax
import jax.numpy as jnp
from jax import lax
from jax.experimental import pallas as pl
from jax.experimental.pallas import tpu as pltpu
from jax.sharding import PartitionSpec as P

MESH = pl.DeviceIdType.MESH
LANES = 128
PAD = 8
FAR, NEAR = 0, 1


def split(value):
    high = value.astype(jnp.bfloat16)
    low = (value - high.astype(jnp.float32)).astype(jnp.bfloat16)
    return high, low


def kernel(
    x_hbm, w_hbm, out, xin, wbuf, w3, sx, acc, mid, pack, got, half, hmain, hhalf, hshift, rmain, rhalf,
    load_x, load_w, row_send, row_recv, frame_send, frame_recv, relay_send, relay_recv,
):
    rows, cols, chans = xin.shape
    layers = wbuf.shape[0]
    tiles = chans // LANES
    both = range(tiles)
    fold = chans // 8
    last = rows - 1
    groups = LANES // fold
    part = cols // groups
    rest = LANES - 2 * fold
    halves = LANES // rest
    frames, bands = lax.axis_size("frame"), lax.axis_size("row")
    t, r = lax.axis_index("frame"), lax.axis_index("row")
    turned = r % 2
    sign = 1 - 2 * turned
    row_to = (r - sign, r + sign)
    has_row = tuple((peer >= 0) & (peer < bands) for peer in row_to)
    edge = (0, last)
    has_frame = (t > 0, t < frames - 1)
    frame_to = (t - 1, t + 1)

    pairs = bands // 2

    def shared(place):
        step = place // 2
        return 4 * (step + (place % 2) * (pairs - 1 - 2 * step)) // pairs

    def takes(place, piece):
        quarters = shared(place)
        return quarters >= 2 if piece == 0 else quarters % 2 == 1

    def within(place):
        return (place >= 0) & (place < bands)

    def relayed(piece):
        return has_row[FAR] & has_row[NEAR] & takes(r, piece)

    onward = r + 2 * sign
    behind = r - 2 * sign

    def relays(piece):
        return has_row[NEAR] & within(onward) & takes(row_to[NEAR], piece)

    def place(row, count):
        return row + turned * (count - 1 - 2 * row)

    loads_x = [pltpu.make_async_copy(x_hbm.at[0, place(q, rows)], xin.at[q], load_x.at[q]) for q in range(rows)]
    loads_w = [
        [pltpu.make_async_copy(w_hbm.at[n, place(d, 3)], wbuf.at[n, d], load_w.at[n, d]) for d in range(3)]
        for n in range(layers)
    ]
    for load in loads_x:
        load.start()

    barrier = pltpu.get_barrier_semaphore()
    count = 0
    for have, axis, peers in ((has_row, "row", row_to), (has_frame, "frame", frame_to)):
        for side in range(2):
            count = count + have[side].astype(jnp.int32)

            @pl.when(have[side])
            def _():
                pl.semaphore_signal(barrier, inc=1, device_id={axis: peers[side]}, device_id_type=MESH)

    for peer in (onward, behind):
        count = count + within(peer).astype(jnp.int32)

        @pl.when(within(peer))
        def _():
            pl.semaphore_signal(barrier, inc=1, device_id={"row": peer}, device_id_type=MESH)

    def maps(layer):
        return xin if layer == 0 else mid.at[layer - 1]

    def row_copy(layer, kind, piece, relay=False):
        if piece == 0:
            upper = pl.ds(LANES, chans - LANES)
            source = maps(layer).at[edge[kind], :, upper]
            target = hmain.at[layer, kind]
        elif piece == 1:
            source, target = half.at[layer, kind], hhalf.at[layer, kind]
        else:
            source = got.at[layer, piece - 2, edge[kind]]
            target = hshift.at[layer, kind, piece - 2]
        return pltpu.make_async_remote_copy(
            src_ref=source,
            dst_ref=(rmain, rhalf)[piece].at[layer] if relay else target,
            send_sem=row_send.at[layer, kind, piece],
            recv_sem=relay_recv.at[layer, piece] if relay else row_recv.at[layer, kind, piece],
            device_id={"row": row_to[NEAR if relay else kind]},
            device_id_type=MESH,
        )

    def relay_copy(layer, piece):
        return pltpu.make_async_remote_copy(
            src_ref=(rmain, rhalf)[piece].at[layer],
            dst_ref=(hmain, hhalf)[piece].at[layer, FAR],
            send_sem=relay_send.at[layer, piece],
            recv_sem=row_recv.at[layer, FAR, piece],
            device_id={"row": onward},
            device_id_type=MESH,
        )

    def start_far(layer, piece):
        @pl.when(relayed(piece))
        def _():
            row_copy(layer, FAR, piece, True).start()

        @pl.when(has_row[FAR] & jnp.logical_not(relayed(piece)))
        def _():
            row_copy(layer, FAR, piece).start()

    def forward(layer, piece, alone=None):
        chosen = relays(piece)
        if alone is not None:
            chosen = chosen & (jnp.logical_not(relays(0)) if alone else relays(0))

        @pl.when(chosen)
        def _():
            row_copy(layer, FAR, piece, True).wait_recv()
            relay_copy(layer, piece).start()

    def sent(kind, piece):
        return has_row[kind] if piece < 2 else has_row[kind] & has_frame[3 - piece]

    def each_piece(layer, kind, pieces, action):
        for piece in pieces:

            @pl.when(sent(kind, piece))
            def _():
                getattr(row_copy(layer, kind, piece), action)()

    blocks = ((0, 1), (1, rows - 2), (last, 1))

    def frame_copy(layer, side, block):
        start, size = blocks[block]
        return pltpu.make_async_remote_copy(
            src_ref=pack.at[layer, side, pl.ds(start, size)],
            dst_ref=got.at[layer, side, pl.ds(start, size)],
            send_sem=frame_send.at[layer, side, block],
            recv_sem=frame_recv.at[layer, side, block],
            device_id={"frame": frame_to[side]},
            device_id_type=MESH,
        )

    def pack_frames(layer, block):
        start, size = blocks[block]
        lane = lax.broadcasted_iota(jnp.int32, (part, LANES), 1)
        for side in range(2):
            for row in range(start, start + size):
                full = None
                for group in range(groups):
                    value = maps(layer)[row, pl.ds(group * part, part), pl.ds(0, LANES)]
                    shift = ((group - side) * fold) % LANES
                    value = pltpu.roll(value, shift, 1) if shift else value
                    full = value if full is None else jnp.where(lane // fold == group, value, full)
                pack[layer, side, row] = full

    def send_frames(layer, block):
        for side in range(2):

            @pl.when(has_frame[side])
            def _():
                frame_copy(layer, side, block).start()

    def take_frames(layer, block):
        for side in range(2):

            @pl.when(has_frame[1 - side])
            def _():
                frame_copy(layer, side, block).wait_recv()

    def pack_half(layer, kind):
        size = cols // halves
        lane = lax.broadcasted_iota(jnp.int32, (size, LANES), 1)
        full = None
        for group in range(halves):
            value = maps(layer)[edge[kind], pl.ds(group * size, size), pl.ds(0, LANES)]
            shift = (group * rest - 2 * fold) % LANES
            value = pltpu.roll(value, shift, 1) if shift else value
            full = value if full is None else jnp.where(lane // rest == group, value, full)
        half[layer, kind] = full

    def put(spot, start, size, tile, value):
        high, low = split(value)
        for n, piece in enumerate((high, low, high)):
            sx[spot, pl.ds(start, size), pl.ds((3 * tile + n) * LANES, LANES)] = piece

    def put_upper(spot, source):
        for tile in range(1, tiles):
            put(spot, 0, cols, tile, source[:, pl.ds((tile - 1) * LANES, LANES)])

    def put_lower(spot, rest_of, shifted):
        lane = lax.broadcasted_iota(jnp.int32, (part, LANES), 1)
        for group in range(groups):
            value = rest_of(group * part)
            for side in range(2):
                moved = shifted(side)
                shift = ((side - group) * fold) % LANES
                moved = pltpu.roll(moved, shift, 1) if shift else moved
                value = jnp.where(lane // fold == side, moved, value)
            put(spot, group * part, part, 0, value)

    def put_row_upper(layer, row):
        put_upper(row + 1, maps(layer).at[row, :, pl.ds(LANES, chans - LANES)])

    def put_row_lower(layer, row):
        put_lower(
            row + 1,
            lambda start: maps(layer)[row, pl.ds(start, part), pl.ds(0, LANES)],
            lambda side: got[layer, side, row],
        )

    def put_halo(layer, kind):
        spot = 0 if kind == FAR else rows + 1
        size = cols // halves

        def rest_of(start):
            group = start // size
            value = hhalf[layer, kind, pl.ds(start - group * size, part)]
            shift = (2 * fold - group * rest) % LANES
            return pltpu.roll(value, shift, 1) if shift else value

        put_lower(spot, rest_of, lambda side: hshift[layer, kind, side])
        put_upper(spot, hmain.at[layer, kind])

    def split_weights(layer):
        for load in loads_w[layer]:
            load.wait()

        def tap(index, carry):
            down, across = index // 3, index % 3
            high, low = split(wbuf[layer, down, across])
            for tile in range(tiles):
                span = slice(tile * LANES, (tile + 1) * LANES)
                base = pl.multiple_of((3 * tile + down) * 3 * LANES, LANES)
                for n, piece in enumerate((high, high, low)):
                    w3[layer, across, pl.ds(base + n * LANES, LANES)] = piece[span]
            return carry

        lax.fori_loop(0, 9, tap, 0)

    def parts_of(sources, seen):
        parts = []
        for row in range(rows):
            downs = [down for down in range(3) if row + down - 1 in sources]
            if downs:
                key = (downs[0], downs[-1] + 1, row in seen)
                if parts and parts[-1][2:] == key and sum(parts[-1][:2]) == row:
                    parts[-1] = (parts[-1][0], parts[-1][1] + 1) + key
                else:
                    parts.append((row, 1) + key)
        seen.update(part[0] + n for part in parts for n in range(part[1]))
        return parts

    def inner(layer, parts, first_tap, taps, which):
        deep = 3 * LANES

        def across(tap, carry):
            for first, count, low, high, add in parts:
                left = jnp.concatenate(
                    [
                        sx[pl.ds(first + down, count), :, pl.ds(tile * deep, deep)].reshape(count * cols, deep)
                        for tile in which
                        for down in range(low, high)
                    ],
                    axis=1,
                )
                right = jnp.concatenate(
                    [
                        w3[layer, tap, pl.ds((3 * tile + low) * deep, (high - low) * deep)]
                        for tile in which
                    ],
                    axis=0,
                )
                total = jnp.dot(left, right, preferred_element_type=jnp.float32)
                total = total.reshape(count, cols, chans)
                if add:
                    acc[layer % 2, tap, pl.ds(first, count), pl.ds(PAD, cols)] += total
                else:
                    acc[layer % 2, tap, pl.ds(first, count), pl.ds(PAD, cols)] = total
            return carry

        lax.fori_loop(first_tap, first_tap + taps, across, 0)

    def outer(layer, kind):
        @pl.when(has_row[kind])
        def _():
            each_piece(layer, kind, range(4), "wait_recv")
            put_halo(layer, kind)

        inner(layer, ((0, 1, 0, 1, True),) if kind == FAR else ((last, 1, 2, 3, True),), 0, 3, both)

    def finish(layer, row):
        part = acc.at[layer % 2, :, row]
        total = part[0, pl.ds(PAD - 1, cols)] + part[1, pl.ds(PAD, cols)]
        total = jnp.maximum(total + part[2, pl.ds(PAD + 1, cols)], 0.0)
        if layer == layers - 1:
            out[place(row, rows)] = total
        else:
            mid[layer, row] = total

    def blank():
        margin = jnp.zeros((2, 3, rows, PAD, chans), jnp.float32)
        acc[:, :, :, pl.ds(0, PAD)] = margin
        acc[:, :, :, pl.ds(PAD + cols, PAD)] = margin
        for kind, spot in ((FAR, 0), (NEAR, rows + 1)):

            @pl.when(jnp.logical_not(has_row[kind]))
            def _():
                sx[spot] = jnp.zeros((cols, 3 * chans), jnp.bfloat16)

        for side in range(2):

            @pl.when(jnp.logical_not(has_frame[1 - side]))
            def _():
                for layer in range(layers):
                    got[layer, side] = jnp.zeros((rows, part, LANES), jnp.float32)
                    for kind in range(2):
                        hshift[layer, kind, side] = jnp.zeros((part, LANES), jnp.float32)

    for load in loads_x:
        load.wait()
    pl.semaphore_wait(barrier, count)
    start_far(0, 0)
    pack_half(0, FAR)
    start_far(0, 1)

    @pl.when(has_row[NEAR] & jnp.logical_not(relayed(0)))
    def _():
        row_copy(0, NEAR, 0).start()

    for per_layer in loads_w:
        for load in per_layer:
            load.start()
    for block in (0, 2, 1):
        pack_frames(0, block)
        send_frames(0, block)
    pack_half(0, NEAR)
    blank()
    for row in range(rows):
        put_row_upper(0, row)
    split_weights(0)
    seen = set()
    parts = parts_of(range(rows), seen)
    inner(0, parts, 0, 1, both[1:])

    @pl.when(has_row[NEAR] & relayed(0))
    def _():
        row_copy(0, NEAR, 0).start()

    each_piece(0, NEAR, range(1, 2), "start")
    take_frames(0, 0)
    each_piece(0, FAR, range(2, 4), "start")
    take_frames(0, 2)
    each_piece(0, NEAR, range(2, 4), "start")
    forward(0, 1, True)
    inner(0, parts, 1, 2, both[1:])
    take_frames(0, 1)
    for row in range(rows):
        put_row_lower(0, row)
    parts = parts_of(range(rows), seen)
    forward(0, 0)
    inner(0, parts, 0, 2, both[:1])
    forward(0, 1, False)
    inner(0, parts, 2, 1, both[:1])
    for layer in range(layers):
        final = layer == layers - 1
        after = layer + 1
        for row in range(1, last):
            finish(layer, row)
        if not final:
            pack_frames(after, 1)
            send_frames(after, 1)
            split_weights(after)
        outer(layer, FAR)
        finish(layer, 0)
        if not final:
            start_far(after, 0)
            pack_half(after, FAR)
            start_far(after, 1)
            pack_frames(after, 0)
            send_frames(after, 0)
        outer(layer, NEAR)
        finish(layer, last)
        if not final:
            each_piece(after, NEAR, range(1), "start")
            pack_frames(after, 2)
            send_frames(after, 2)
            pack_half(after, NEAR)
            each_piece(after, NEAR, range(1, 2), "start")
            take_frames(after, 1)
            for row in range(1, last):
                put_row_upper(after, row)
                put_row_lower(after, row)
            seen = set()
            parts = parts_of(range(1, last), seen)
            inner(after, parts, 0, 2, both)
            take_frames(after, 0)
            each_piece(after, FAR, range(2, 4), "start")
            forward(after, 1, True)
            forward(after, 0)
            inner(after, parts, 2, 1, both)
            take_frames(after, 2)
            each_piece(after, NEAR, range(2, 4), "start")
            put_row_upper(after, 0)
            put_row_lower(after, 0)
            inner(after, parts_of((0,), seen), 0, 3, both)
            forward(after, 1, False)
            put_row_upper(after, last)
            put_row_lower(after, last)
            inner(after, parts_of((last,), seen), 0, 3, both)

    for layer in range(layers):
        for kind in range(2):
            each_piece(layer, kind, range(4), "wait_send")
        for piece in range(2):

            @pl.when(relays(piece))
            def _():
                relay_copy(layer, piece).wait_send()

        for side in range(2):
            for block in range(len(blocks)):

                @pl.when(has_frame[side])
                def _():
                    frame_copy(layer, side, block).wait_send()


def store(y_ref, o_hbm, sem):
    copies = [pltpu.make_async_copy(y_ref.at[n], o_hbm.at[0, n], sem.at[n]) for n in range(y_ref.shape[0])]
    for copy in copies:
        copy.start()
    for copy in copies:
        copy.wait()


def local(features, conv_weight):
    _, rows, cols, chans = features.shape
    layers = conv_weight.shape[0]
    fold = chans // 8
    part = cols // (LANES // fold)
    halved = cols // (LANES // (LANES - 2 * fold))
    f32, bf16 = jnp.float32, jnp.bfloat16
    dma = pltpu.SemaphoreType.DMA
    result = pl.pallas_call(
        kernel,
        out_shape=pltpu.VMEM((rows, cols, chans), f32),
        in_specs=[pl.BlockSpec(memory_space=pl.ANY)] * 2,
        out_specs=pl.BlockSpec(memory_space=pltpu.VMEM),
        scratch_shapes=[
            pltpu.VMEM((rows, cols, chans), f32),
            pltpu.VMEM(conv_weight.shape, f32),
            pltpu.VMEM((layers, 3, 9 * chans, chans), bf16),
            pltpu.VMEM((rows + 2, cols, 3 * chans), bf16),
            pltpu.VMEM((2, 3, rows, cols + 2 * PAD, chans), f32),
            pltpu.VMEM((layers - 1, rows, cols, chans), f32),
            pltpu.VMEM((layers, 2, rows, part, LANES), f32),
            pltpu.VMEM((layers, 2, rows, part, LANES), f32),
            pltpu.VMEM((layers, 2, halved, LANES), f32),
            pltpu.VMEM((layers, 2, cols, chans - LANES), f32),
            pltpu.VMEM((layers, 2, halved, LANES), f32),
            pltpu.VMEM((layers, 2, 2, part, LANES), f32),
            pltpu.VMEM((layers, cols, chans - LANES), f32),
            pltpu.VMEM((layers, halved, LANES), f32),
            dma((rows,)),
            dma((layers, 3)),
            dma((layers, 2, 4)),
            dma((layers, 2, 4)),
            dma((layers, 2, 3)),
            dma((layers, 2, 3)),
            dma((layers, 2)),
            dma((layers, 2)),
        ],
        compiler_params=pltpu.CompilerParams(
            collective_id=0, has_side_effects=True, vmem_limit_bytes=62 * 1024 * 1024
        ),
    )(features, conv_weight)
    return pl.pallas_call(
        store,
        out_shape=jax.ShapeDtypeStruct(features.shape, f32),
        in_specs=[pl.BlockSpec(memory_space=pltpu.VMEM)],
        out_specs=pl.BlockSpec(memory_space=pl.ANY),
        scratch_shapes=[dma((rows,))],
        compiler_params=pltpu.CompilerParams(vmem_limit_bytes=2 * 1024 * 1024),
    )(result)


def solution(mesh):
    placed = (P("frame", "row", None, None), P())
    return jax.shard_map(
        local, mesh=mesh, in_specs=placed, out_specs=P("frame", "row", None, None), check_vma=False
    )
```

```python
import jax
import jax.numpy as jnp
from jax import lax
from jax.experimental import pallas as pl
from jax.experimental.pallas import tpu as pltpu
from jax.sharding import PartitionSpec as P

MESH = pl.DeviceIdType.MESH
LANES = 128
PAD = 8
FAR, NEAR = 0, 1


def split(value):
    high = value.astype(jnp.bfloat16)
    low = (value - high.astype(jnp.float32)).astype(jnp.bfloat16)
    return high, low


def kernel(
    x_hbm, w_hbm, out, xin, wbuf, w3, sx, acc, mid, pack, got, half, hmain, hhalf, hshift, rmain, rhalf,
    load_x, load_w, row_send, row_recv, frame_send, frame_recv, relay_send, relay_recv,
):
    rows, cols, chans = xin.shape
    layers = wbuf.shape[0]
    tiles = chans // LANES
    both = range(tiles)
    fold = chans // 8
    last = rows - 1
    groups = LANES // fold
    part = cols // groups
    rest = LANES - 2 * fold
    halves = LANES // rest
    frames, bands = lax.axis_size("frame"), lax.axis_size("row")
    t, r = lax.axis_index("frame"), lax.axis_index("row")
    turned = r % 2
    sign = 1 - 2 * turned
    row_to = (r - sign, r + sign)
    has_row = tuple((peer >= 0) & (peer < bands) for peer in row_to)
    edge = (0, last)
    has_frame = (t > 0, t < frames - 1)
    frame_to = (t - 1, t + 1)

    pairs = bands // 2

    def shared(place):
        step = place // 2
        return 4 * (step + (place % 2) * (pairs - 1 - 2 * step)) // pairs

    def takes(place, piece):
        return shared(place) > piece

    def within(place):
        return (place >= 0) & (place < bands)

    def relayed(piece):
        return has_row[FAR] & has_row[NEAR] & takes(r, piece)

    onward = r + 2 * sign
    behind = r - 2 * sign

    def relays(piece):
        return has_row[NEAR] & within(onward) & takes(row_to[NEAR], piece)

    def place(row, count):
        return row + turned * (count - 1 - 2 * row)

    loads_x = [pltpu.make_async_copy(x_hbm.at[0, place(q, rows)], xin.at[q], load_x) for q in range(rows)]
    loads_w = [
        [pltpu.make_async_copy(w_hbm.at[n, place(d, 3)], wbuf.at[n, d], load_w.at[n]) for d in range(3)]
        for n in range(layers)
    ]
    for load in loads_x:
        load.start()

    barrier = pltpu.get_barrier_semaphore()
    count = 0
    for have, axis, peers in ((has_row, "row", row_to), (has_frame, "frame", frame_to)):
        for side in range(2):
            count = count + have[side].astype(jnp.int32)

            @pl.when(have[side])
            def _():
                pl.semaphore_signal(barrier, inc=1, device_id={axis: peers[side]}, device_id_type=MESH)

    for peer in (onward, behind):
        count = count + within(peer).astype(jnp.int32)

        @pl.when(within(peer))
        def _():
            pl.semaphore_signal(barrier, inc=1, device_id={"row": peer}, device_id_type=MESH)

    def maps(layer):
        return xin if layer == 0 else mid.at[layer - 1]

    def section(piece):
        return pl.ds(piece * (cols // 2), cols // 2)

    def row_copy(layer, kind, piece, relay=False):
        if piece < 2:
            source = maps(layer).at[edge[kind], section(piece), pl.ds(LANES, chans - LANES)]
            target = (rmain.at[layer] if relay else hmain.at[layer, kind]).at[section(piece)]
        elif piece == 2:
            source = half.at[layer, kind]
            target = rhalf.at[layer] if relay else hhalf.at[layer, kind]
        else:
            source = got.at[layer, piece - 3, edge[kind]]
            target = hshift.at[layer, kind, piece - 3]
        return pltpu.make_async_remote_copy(
            src_ref=source,
            dst_ref=target,
            send_sem=row_send.at[kind, piece],
            recv_sem=relay_recv.at[layer, piece] if relay else row_recv.at[layer, kind, piece],
            device_id={"row": row_to[NEAR if relay else kind]},
            device_id_type=MESH,
        )

    def relay_copy(layer, piece):
        if piece < 2:
            source, target = (ref.at[section(piece)] for ref in (rmain.at[layer], hmain.at[layer, FAR]))
        else:
            source, target = rhalf.at[layer], hhalf.at[layer, FAR]
        return pltpu.make_async_remote_copy(
            src_ref=source,
            dst_ref=target,
            send_sem=relay_send.at[piece],
            recv_sem=row_recv.at[layer, FAR, piece],
            device_id={"row": onward},
            device_id_type=MESH,
        )

    def start_far(layer, piece):
        @pl.when(relayed(piece))
        def _():
            row_copy(layer, FAR, piece, True).start()

        @pl.when(has_row[FAR] & jnp.logical_not(relayed(piece)))
        def _():
            row_copy(layer, FAR, piece).start()

    def drain_frames(layer, block):
        for side in range(2):

            @pl.when(has_frame[side])
            def _():
                frame_copy(layer, side, block).wait_send()

    def drain(layer):
        for kind in range(2):
            each_piece(layer, kind, range(5), "wait_send")
        for piece in range(3):

            @pl.when(relays(piece))
            def _():
                relay_copy(layer, piece).wait_send()

        for block in range(len(blocks)):
            drain_frames(layer, block)

    def start_near(layer, late):
        @pl.when(has_row[NEAR] & (relayed(1) if late else jnp.logical_not(relayed(1))))
        def _():
            for piece in range(3):
                row_copy(layer, NEAR, piece).start()

    def forward(layer, piece):
        @pl.when(relays(piece))
        def _():
            row_copy(layer, FAR, piece, True).wait_recv()
            relay_copy(layer, piece).start()

    def sent(kind, piece):
        return has_row[kind] if piece < 3 else has_row[kind] & has_frame[4 - piece]

    def each_piece(layer, kind, pieces, action):
        for piece in pieces:

            @pl.when(sent(kind, piece))
            def _():
                getattr(row_copy(layer, kind, piece), action)()

    blocks = ((0, 1), (1, rows - 2), (last, 1))

    def frame_copy(layer, side, block):
        start, size = blocks[block]
        return pltpu.make_async_remote_copy(
            src_ref=pack.at[layer, side, pl.ds(start, size)],
            dst_ref=got.at[layer, side, pl.ds(start, size)],
            send_sem=frame_send.at[side, block],
            recv_sem=frame_recv.at[layer, side, block],
            device_id={"frame": frame_to[side]},
            device_id_type=MESH,
        )

    def pack_frames(layer, block):
        start, size = blocks[block]
        lane = lax.broadcasted_iota(jnp.int32, (part, LANES), 1)
        for side in range(2):
            for row in range(start, start + size):
                full = None
                for group in range(groups):
                    value = maps(layer)[row, pl.ds(group * part, part), pl.ds(0, LANES)]
                    shift = ((group - side) * fold) % LANES
                    value = pltpu.roll(value, shift, 1) if shift else value
                    full = value if full is None else jnp.where(lane // fold == group, value, full)
                pack[layer, side, row] = full

    def send_frames(layer, block):
        for side in range(2):

            @pl.when(has_frame[side])
            def _():
                frame_copy(layer, side, block).start()

    def take_frames(layer, block):
        for side in range(2):

            @pl.when(has_frame[1 - side])
            def _():
                frame_copy(layer, side, block).wait_recv()

    def pack_half(layer, kind):
        size = cols // halves
        lane = lax.broadcasted_iota(jnp.int32, (size, LANES), 1)
        full = None
        for group in range(halves):
            value = maps(layer)[edge[kind], pl.ds(group * size, size), pl.ds(0, LANES)]
            shift = (group * rest - 2 * fold) % LANES
            value = pltpu.roll(value, shift, 1) if shift else value
            full = value if full is None else jnp.where(lane // rest == group, value, full)
        half[layer, kind] = full

    def put(spot, start, size, tile, value):
        high, low = split(value)
        for n, piece in enumerate((high, low, high)):
            sx[spot, pl.ds(start, size), pl.ds((3 * tile + n) * LANES, LANES)] = piece

    def put_upper(spot, source):
        for tile in range(1, tiles):
            put(spot, 0, cols, tile, source[:, pl.ds((tile - 1) * LANES, LANES)])

    def put_lower(spot, rest_of, shifted):
        lane = lax.broadcasted_iota(jnp.int32, (part, LANES), 1)
        for group in range(groups):
            value = rest_of(group * part)
            for side in range(2):
                moved = shifted(side)
                shift = ((side - group) * fold) % LANES
                moved = pltpu.roll(moved, shift, 1) if shift else moved
                value = jnp.where(lane // fold == side, moved, value)
            put(spot, group * part, part, 0, value)

    def put_row_upper(layer, row):
        put_upper(row + 1, maps(layer).at[row, :, pl.ds(LANES, chans - LANES)])

    def put_row_lower(layer, row):
        put_lower(
            row + 1,
            lambda start: maps(layer)[row, pl.ds(start, part), pl.ds(0, LANES)],
            lambda side: got[layer, side, row],
        )

    def put_halo(layer, kind):
        spot = 0 if kind == FAR else rows + 1
        size = cols // halves

        def rest_of(start):
            group = start // size
            value = hhalf[layer, kind, pl.ds(start - group * size, part)]
            shift = (2 * fold - group * rest) % LANES
            return pltpu.roll(value, shift, 1) if shift else value

        put_lower(spot, rest_of, lambda side: hshift[layer, kind, side])

    def split_weights(layer):
        pltpu.make_async_copy(w_hbm.at[layer], wbuf.at[layer], load_w.at[layer]).wait()

        def tap(index, carry):
            down, across = index // 3, index % 3
            high, low = split(wbuf[layer, down, across])
            for tile in range(tiles):
                span = slice(tile * LANES, (tile + 1) * LANES)
                base = pl.multiple_of((3 * tile + down) * 3 * LANES, LANES)
                for n, piece in enumerate((high, high, low)):
                    w3[layer, across, pl.ds(base + n * LANES, LANES)] = piece[span]
            return carry

        lax.fori_loop(0, 9, tap, 0)

    def parts_of(sources, seen):
        parts = []
        for row in range(rows):
            downs = [down for down in range(3) if row + down - 1 in sources]
            if downs:
                key = (downs[0], downs[-1] + 1, row in seen)
                if parts and parts[-1][2:] == key and sum(parts[-1][:2]) == row:
                    parts[-1] = (parts[-1][0], parts[-1][1] + 1) + key
                else:
                    parts.append((row, 1) + key)
        seen.update(part[0] + n for part in parts for n in range(part[1]))
        return parts

    def inner(layer, parts, first_tap, taps, which):
        deep = 3 * LANES

        def across(tap, carry):
            for first, count, low, high, add in parts:
                left = jnp.concatenate(
                    [
                        sx[pl.ds(first + down, count), :, pl.ds(tile * deep, deep)].reshape(count * cols, deep)
                        for tile in which
                        for down in range(low, high)
                    ],
                    axis=1,
                )
                right = jnp.concatenate(
                    [
                        w3[layer, tap, pl.ds((3 * tile + low) * deep, (high - low) * deep)]
                        for tile in which
                    ],
                    axis=0,
                )
                total = jnp.dot(left, right, preferred_element_type=jnp.float32)
                total = total.reshape(count, cols, chans)
                if add:
                    acc[layer % 2, tap, pl.ds(first, count), pl.ds(PAD, cols)] += total
                else:
                    acc[layer % 2, tap, pl.ds(first, count), pl.ds(PAD, cols)] = total
            return carry

        lax.fori_loop(first_tap, first_tap + taps, across, 0)

    def outer(layer, kind):
        spot = 0 if kind == FAR else rows + 1
        parts = ((0, 1, 0, 1, True),) if kind == FAR else ((last, 1, 2, 3, True),)
        steps = (both[1:], both[:1]) if layer == layers - 1 and kind == NEAR else (both,)
        for step in steps:

            @pl.when(has_row[kind])
            def _():
                if 1 in step:
                    each_piece(layer, kind, range(2), "wait_recv")
                    put_upper(spot, hmain.at[layer, kind])
                if 0 in step:
                    each_piece(layer, kind, range(2, 5), "wait_recv")
                    put_halo(layer, kind)

            inner(layer, parts, 0, 3, step)

    def finish(layer, row):
        part = acc.at[layer % 2, :, row]
        total = part[0, pl.ds(PAD - 1, cols)] + part[1, pl.ds(PAD, cols)]
        total = jnp.maximum(total + part[2, pl.ds(PAD + 1, cols)], 0.0)
        if layer == layers - 1:
            out[place(row, rows)] = total
        else:
            mid[layer, row] = total

    def blank():
        margin = jnp.zeros((2, 3, rows, PAD, chans), jnp.float32)
        acc[:, :, :, pl.ds(0, PAD)] = margin
        acc[:, :, :, pl.ds(PAD + cols, PAD)] = margin
        for kind, spot in ((FAR, 0), (NEAR, rows + 1)):

            @pl.when(jnp.logical_not(has_row[kind]))
            def _():
                sx[spot] = jnp.zeros((cols, 3 * chans), jnp.bfloat16)

        for side in range(2):

            @pl.when(jnp.logical_not(has_frame[1 - side]))
            def _():
                for layer in range(layers):
                    got[layer, side] = jnp.zeros((rows, part, LANES), jnp.float32)
                    for kind in range(2):
                        hshift[layer, kind, side] = jnp.zeros((part, LANES), jnp.float32)

    pltpu.make_async_copy(x_hbm.at[0], xin, load_x).wait()
    pl.semaphore_wait(barrier, count)
    start_far(0, 0)
    start_far(0, 1)
    pack_half(0, FAR)
    start_far(0, 2)
    for per_layer in loads_w:
        for load in per_layer:
            load.start()
    for block in (0, 2, 1):
        pack_frames(0, block)
        send_frames(0, block)
    pack_half(0, NEAR)
    start_near(0, False)
    blank()
    for row in range(rows):
        put_row_upper(0, row)
    split_weights(0)
    seen = set()
    parts = parts_of(range(rows), seen)
    inner(0, parts, 0, 1, both[1:])
    start_near(0, True)
    take_frames(0, 0)
    each_piece(0, FAR, range(3, 5), "start")
    take_frames(0, 2)
    each_piece(0, NEAR, range(3, 5), "start")
    inner(0, parts, 1, 1, both[1:])
    forward(0, 0)
    inner(0, parts, 2, 1, both[1:])
    take_frames(0, 1)
    for row in range(rows):
        put_row_lower(0, row)
    parts = parts_of(range(rows), seen)
    forward(0, 1)
    inner(0, parts, 0, 2, both[:1])
    forward(0, 2)
    inner(0, parts, 2, 1, both[:1])
    for layer in range(layers):
        final = layer == layers - 1
        after = layer + 1
        for row in range(1, last):
            finish(layer, row)
        if not final:
            pack_frames(after, 1)
            drain_frames(layer, 1)
            send_frames(after, 1)
            split_weights(after)
        outer(layer, FAR)
        finish(layer, 0)
        if not final:
            each_piece(layer, FAR, range(5), "wait_send")
            start_far(after, 0)
            start_far(after, 1)
            pack_half(after, FAR)
            start_far(after, 2)
            pack_frames(after, 0)
            drain_frames(layer, 0)
            send_frames(after, 0)
        outer(layer, NEAR)
        finish(layer, last)
        if not final:
            each_piece(layer, NEAR, range(5), "wait_send")
            each_piece(after, NEAR, range(2), "start")
            pack_frames(after, 2)
            drain_frames(layer, 2)
            send_frames(after, 2)
            pack_half(after, NEAR)
            each_piece(after, NEAR, range(2, 3), "start")
            take_frames(after, 1)
            for row in range(1, last):
                put_row_upper(after, row)
                put_row_lower(after, row)
            seen = set()
            parts = parts_of(range(1, last), seen)
            inner(after, parts, 0, 2, both)
            for piece in range(3):

                @pl.when(relays(piece))
                def _():
                    relay_copy(layer, piece).wait_send()

            take_frames(after, 0)
            each_piece(after, FAR, range(3, 5), "start")
            forward(after, 0)
            inner(after, parts, 2, 1, both)
            take_frames(after, 2)
            each_piece(after, NEAR, range(3, 5), "start")
            forward(after, 1)
            put_row_upper(after, 0)
            put_row_lower(after, 0)
            inner(after, parts_of((0,), seen), 0, 3, both)
            forward(after, 2)
            put_row_upper(after, last)
            put_row_lower(after, last)
            inner(after, parts_of((last,), seen), 0, 3, both)

    drain(layers - 1)


def store(y_ref, o_hbm, sem):
    copies = [pltpu.make_async_copy(y_ref.at[n], o_hbm.at[0, n], sem.at[n]) for n in range(y_ref.shape[0])]
    for copy in copies:
        copy.start()
    for copy in copies:
        copy.wait()


def local(features, conv_weight):
    _, rows, cols, chans = features.shape
    layers = conv_weight.shape[0]
    fold = chans // 8
    part = cols // (LANES // fold)
    halved = cols // (LANES // (LANES - 2 * fold))
    f32, bf16 = jnp.float32, jnp.bfloat16
    dma = pltpu.SemaphoreType.DMA
    result = pl.pallas_call(
        kernel,
        out_shape=pltpu.VMEM((rows, cols, chans), f32),
        in_specs=[pl.BlockSpec(memory_space=pl.ANY)] * 2,
        out_specs=pl.BlockSpec(memory_space=pltpu.VMEM),
        scratch_shapes=[
            pltpu.VMEM((rows, cols, chans), f32),
            pltpu.VMEM(conv_weight.shape, f32),
            pltpu.VMEM((layers, 3, 9 * chans, chans), bf16),
            pltpu.VMEM((rows + 2, cols, 3 * chans), bf16),
            pltpu.VMEM((2, 3, rows, cols + 2 * PAD, chans), f32),
            pltpu.VMEM((layers - 1, rows, cols, chans), f32),
            pltpu.VMEM((layers, 2, rows, part, LANES), f32),
            pltpu.VMEM((layers, 2, rows, part, LANES), f32),
            pltpu.VMEM((layers, 2, halved, LANES), f32),
            pltpu.VMEM((layers, 2, cols, chans - LANES), f32),
            pltpu.VMEM((layers, 2, halved, LANES), f32),
            pltpu.VMEM((layers, 2, 2, part, LANES), f32),
            pltpu.VMEM((layers, cols, chans - LANES), f32),
            pltpu.VMEM((layers, halved, LANES), f32),
            dma,
            dma((layers,)),
            dma((2, 5)),
            dma((layers, 2, 5)),
            dma((2, 3)),
            dma((layers, 2, 3)),
            dma((3,)),
            dma((layers, 3)),
        ],
        compiler_params=pltpu.CompilerParams(
            collective_id=0, has_side_effects=True, vmem_limit_bytes=62 * 1024 * 1024
        ),
    )(features, conv_weight)
    return pl.pallas_call(
        store,
        out_shape=jax.ShapeDtypeStruct(features.shape, f32),
        in_specs=[pl.BlockSpec(memory_space=pltpu.VMEM)],
        out_specs=pl.BlockSpec(memory_space=pl.ANY),
        scratch_shapes=[dma((rows,))],
        compiler_params=pltpu.CompilerParams(vmem_limit_bytes=2 * 1024 * 1024),
    )(result)


def solution(mesh):
    placed = (P("frame", "row", None, None), P())
    return jax.shard_map(
        local, mesh=mesh, in_specs=placed, out_specs=P("frame", "row", None, None), check_vma=False
    )
```

```python
import jax
import jax.numpy as jnp
from jax import lax
from jax.experimental import pallas as pl
from jax.experimental.pallas import tpu as pltpu
from jax.sharding import PartitionSpec as P

MESH = pl.DeviceIdType.MESH
LANES = 128
PAD = 8
FAR, NEAR = 0, 1


def split(value):
    high = value.astype(jnp.bfloat16)
    low = (value - high.astype(jnp.float32)).astype(jnp.bfloat16)
    return high, low


def kernel(
    x_hbm, w_hbm, out, w3, sx, acc, xin, wbuf, mid, pack, got, half, hmain, hhalf, hshift, rmain, rhalf,
    load_x, load_w, row_send, row_recv, frame_send, frame_recv, relay_send, relay_recv,
):
    rows, cols, chans = xin.shape
    layers = wbuf.shape[0]
    tiles = chans // LANES
    both = range(tiles)
    fold = chans // 8
    last = rows - 1
    groups = LANES // fold
    part = cols // groups
    rest = LANES - 2 * fold
    halves = LANES // rest
    frames, bands = lax.axis_size("frame"), lax.axis_size("row")
    t, r = lax.axis_index("frame"), lax.axis_index("row")
    turned = r % 2
    sign = 1 - 2 * turned
    row_to = (r - sign, r + sign)
    has_row = tuple((peer >= 0) & (peer < bands) for peer in row_to)
    edge = (0, last)
    has_frame = (t > 0, t < frames - 1)
    frame_to = (t - 1, t + 1)

    pairs = bands // 2

    def shared(place):
        step = place // 2
        return 4 * (step + (place % 2) * (pairs - 1 - 2 * step)) // pairs

    def takes(place, piece):
        return shared(place) > piece

    def within(place):
        return (place >= 0) & (place < bands)

    def relayed(piece):
        return has_row[FAR] & has_row[NEAR] & takes(r, piece)

    onward = r + 2 * sign
    behind = r - 2 * sign

    def relays(piece):
        return has_row[NEAR] & within(onward) & takes(row_to[NEAR], piece)

    def place(row, count):
        return row + turned * (count - 1 - 2 * row)

    loads_x = [pltpu.make_async_copy(x_hbm.at[0, place(q, rows)], xin.at[q], load_x) for q in range(rows)]
    loads_w = [
        [pltpu.make_async_copy(w_hbm.at[n, place(d, 3)], wbuf.at[n, d], load_w.at[n]) for d in range(3)]
        for n in range(layers)
    ]
    for load in loads_x:
        load.start()

    barrier = pltpu.get_barrier_semaphore()
    count = 0
    for have, axis, peers in ((has_row, "row", row_to), (has_frame, "frame", frame_to)):
        for side in range(2):
            count = count + have[side].astype(jnp.int32)

            @pl.when(have[side])
            def _():
                pl.semaphore_signal(barrier, inc=1, device_id={axis: peers[side]}, device_id_type=MESH)

    for peer in (onward, behind):
        count = count + within(peer).astype(jnp.int32)

        @pl.when(within(peer))
        def _():
            pl.semaphore_signal(barrier, inc=1, device_id={"row": peer}, device_id_type=MESH)

    def maps(layer):
        return xin if layer == 0 else mid.at[layer - 1]

    def section(piece):
        return pl.ds(piece * (cols // 2), cols // 2)

    def row_copy(layer, kind, piece, relay=False):
        if piece < 2:
            source = maps(layer).at[edge[kind], section(piece), pl.ds(LANES, chans - LANES)]
            target = (rmain.at[layer] if relay else hmain.at[layer, kind]).at[section(piece)]
        elif piece == 2:
            source = half.at[layer, kind]
            target = rhalf.at[layer] if relay else hhalf.at[layer, kind]
        else:
            source = got.at[layer, piece - 3, edge[kind]]
            target = hshift.at[layer, kind, piece - 3]
        return pltpu.make_async_remote_copy(
            src_ref=source,
            dst_ref=target,
            send_sem=row_send.at[kind, piece],
            recv_sem=relay_recv.at[layer, piece] if relay else row_recv.at[layer, kind, piece],
            device_id={"row": row_to[NEAR if relay else kind]},
            device_id_type=MESH,
        )

    def relay_copy(layer, piece):
        if piece < 2:
            source, target = (ref.at[section(piece)] for ref in (rmain.at[layer], hmain.at[layer, FAR]))
        else:
            source, target = rhalf.at[layer], hhalf.at[layer, FAR]
        return pltpu.make_async_remote_copy(
            src_ref=source,
            dst_ref=target,
            send_sem=relay_send.at[piece],
            recv_sem=row_recv.at[layer, FAR, piece],
            device_id={"row": onward},
            device_id_type=MESH,
        )

    def start_far(layer, piece):
        @pl.when(relayed(piece))
        def _():
            row_copy(layer, FAR, piece, True).start()

        @pl.when(has_row[FAR] & jnp.logical_not(relayed(piece)))
        def _():
            row_copy(layer, FAR, piece).start()

    def drain_frames(layer, block):
        for side in range(2):

            @pl.when(has_frame[side])
            def _():
                frame_copy(layer, side, block).wait_send()

    def drain(layer):
        for kind in range(2):
            each_piece(layer, kind, range(5), "wait_send")
        for piece in range(3):

            @pl.when(relays(piece))
            def _():
                relay_copy(layer, piece).wait_send()

        for block in range(len(blocks)):
            drain_frames(layer, block)

    def start_near(layer, late):
        @pl.when(has_row[NEAR] & (relayed(1) if late else jnp.logical_not(relayed(1))))
        def _():
            for piece in range(3):
                row_copy(layer, NEAR, piece).start()

    def forward(layer, piece):
        @pl.when(relays(piece))
        def _():
            row_copy(layer, FAR, piece, True).wait_recv()
            relay_copy(layer, piece).start()

    def sent(kind, piece):
        return has_row[kind] if piece < 3 else has_row[kind] & has_frame[4 - piece]

    def each_piece(layer, kind, pieces, action):
        for piece in pieces:

            @pl.when(sent(kind, piece))
            def _():
                getattr(row_copy(layer, kind, piece), action)()

    blocks = ((0, 1), (1, rows - 2), (last, 1))

    def frame_copy(layer, side, block):
        start, size = blocks[block]
        return pltpu.make_async_remote_copy(
            src_ref=pack.at[layer, side, pl.ds(start, size)],
            dst_ref=got.at[layer, side, pl.ds(start, size)],
            send_sem=frame_send.at[side, block],
            recv_sem=frame_recv.at[layer, side, block],
            device_id={"frame": frame_to[side]},
            device_id_type=MESH,
        )

    def pack_frames(layer, block):
        start, size = blocks[block]
        lane = lax.broadcasted_iota(jnp.int32, (part, LANES), 1)
        for side in range(2):
            for row in range(start, start + size):
                full = None
                for group in range(groups):
                    value = maps(layer)[row, pl.ds(group * part, part), pl.ds(0, LANES)]
                    shift = ((group - side) * fold) % LANES
                    value = pltpu.roll(value, shift, 1) if shift else value
                    full = value if full is None else jnp.where(lane // fold == group, value, full)
                pack[layer, side, row] = full

    def send_frames(layer, block):
        for side in range(2):

            @pl.when(has_frame[side])
            def _():
                frame_copy(layer, side, block).start()

    def take_frames(layer, block):
        for side in range(2):

            @pl.when(has_frame[1 - side])
            def _():
                frame_copy(layer, side, block).wait_recv()

    def pack_half(layer, kind):
        size = cols // halves
        lane = lax.broadcasted_iota(jnp.int32, (size, LANES), 1)
        full = None
        for group in range(halves):
            value = maps(layer)[edge[kind], pl.ds(group * size, size), pl.ds(0, LANES)]
            shift = (group * rest - 2 * fold) % LANES
            value = pltpu.roll(value, shift, 1) if shift else value
            full = value if full is None else jnp.where(lane // rest == group, value, full)
        half[layer, kind] = full

    def put(spot, start, size, tile, value):
        high, low = split(value)
        for n, piece in enumerate((high, low, high)):
            sx[spot, pl.ds(start, size), pl.ds((3 * tile + n) * LANES, LANES)] = piece

    def put_upper(spot, source):
        for tile in range(1, tiles):
            put(spot, 0, cols, tile, source[:, pl.ds((tile - 1) * LANES, LANES)])

    def put_lower(spot, rest_of, shifted):
        lane = lax.broadcasted_iota(jnp.int32, (part, LANES), 1)
        for group in range(groups):
            value = rest_of(group * part)
            for side in range(2):
                moved = shifted(side)
                shift = ((side - group) * fold) % LANES
                moved = pltpu.roll(moved, shift, 1) if shift else moved
                value = jnp.where(lane // fold == side, moved, value)
            put(spot, group * part, part, 0, value)

    def put_row_upper(layer, row):
        put_upper(row + 1, maps(layer).at[row, :, pl.ds(LANES, chans - LANES)])

    def put_row_lower(layer, row):
        put_lower(
            row + 1,
            lambda start: maps(layer)[row, pl.ds(start, part), pl.ds(0, LANES)],
            lambda side: got[layer, side, row],
        )

    def put_halo(layer, kind):
        spot = 0 if kind == FAR else rows + 1
        size = cols // halves

        def rest_of(start):
            group = start // size
            value = hhalf[layer, kind, pl.ds(start - group * size, part)]
            shift = (2 * fold - group * rest) % LANES
            return pltpu.roll(value, shift, 1) if shift else value

        put_lower(spot, rest_of, lambda side: hshift[layer, kind, side])

    def split_weights(layer):
        pltpu.make_async_copy(w_hbm.at[layer], wbuf.at[layer], load_w.at[layer]).wait()

        def tap(index, carry):
            down, across = index // 3, index % 3
            high, low = split(wbuf[layer, down, across])
            for tile in range(tiles):
                span = slice(tile * LANES, (tile + 1) * LANES)
                base = pl.multiple_of((3 * tile + down) * 3 * LANES, LANES)
                for n, piece in enumerate((high, high, low)):
                    w3[layer, across, pl.ds(base + n * LANES, LANES)] = piece[span]
            return carry

        lax.fori_loop(0, 9, tap, 0)

    def parts_of(sources, seen):
        parts = []
        for row in range(rows):
            downs = [down for down in range(3) if row + down - 1 in sources]
            if downs:
                key = (downs[0], downs[-1] + 1, row in seen)
                if parts and parts[-1][2:] == key and sum(parts[-1][:2]) == row:
                    parts[-1] = (parts[-1][0], parts[-1][1] + 1) + key
                else:
                    parts.append((row, 1) + key)
        seen.update(part[0] + n for part in parts for n in range(part[1]))
        return parts

    def inner(layer, parts, first_tap, taps, which):
        deep = 3 * LANES

        def across(tap, carry):
            for first, count, low, high, add in parts:
                left = jnp.concatenate(
                    [
                        sx[pl.ds(first + down, count), :, pl.ds(tile * deep, deep)].reshape(count * cols, deep)
                        for tile in which
                        for down in range(low, high)
                    ],
                    axis=1,
                )
                right = jnp.concatenate(
                    [
                        w3[layer, tap, pl.ds((3 * tile + low) * deep, (high - low) * deep)]
                        for tile in which
                    ],
                    axis=0,
                )
                total = jnp.dot(left, right, preferred_element_type=jnp.float32)
                total = total.reshape(count, cols, chans)
                if add:
                    acc[layer % 2, tap, pl.ds(first, count), pl.ds(PAD, cols)] += total
                else:
                    acc[layer % 2, tap, pl.ds(first, count), pl.ds(PAD, cols)] = total
            return carry

        lax.fori_loop(first_tap, first_tap + taps, across, 0)

    def outer(layer, kind):
        spot = 0 if kind == FAR else rows + 1
        parts = ((0, 1, 0, 1, True),) if kind == FAR else ((last, 1, 2, 3, True),)
        steps = (both[1:], both[:1]) if layer == layers - 1 and kind == NEAR else (both,)
        for step in steps:

            @pl.when(has_row[kind])
            def _():
                if 1 in step:
                    each_piece(layer, kind, range(2), "wait_recv")
                    put_upper(spot, hmain.at[layer, kind])
                if 0 in step:
                    each_piece(layer, kind, range(2, 5), "wait_recv")
                    put_halo(layer, kind)

            if steps == (both,) or 0 not in step:
                inner(layer, parts, 0, 3, step)

    def finish(layer, row):
        part = acc.at[layer % 2, :, row]
        total = part[0, pl.ds(PAD - 1, cols)] + part[1, pl.ds(PAD, cols)]
        total = jnp.maximum(total + part[2, pl.ds(PAD + 1, cols)], 0.0)
        if layer == layers - 1:
            out[place(row, rows)] = total
        else:
            mid[layer, row] = total

    def blank():
        margin = jnp.zeros((2, 3, rows, PAD, chans), jnp.float32)
        acc[:, :, :, pl.ds(0, PAD)] = margin
        acc[:, :, :, pl.ds(PAD + cols, PAD)] = margin
        for kind, spot in ((FAR, 0), (NEAR, rows + 1)):

            @pl.when(jnp.logical_not(has_row[kind]))
            def _():
                sx[spot] = jnp.zeros((cols, 3 * chans), jnp.bfloat16)

        for side in range(2):

            @pl.when(jnp.logical_not(has_frame[1 - side]))
            def _():
                for layer in range(layers):
                    got[layer, side] = jnp.zeros((rows, part, LANES), jnp.float32)
                    for kind in range(2):
                        hshift[layer, kind, side] = jnp.zeros((part, LANES), jnp.float32)

    pltpu.make_async_copy(x_hbm.at[0], xin, load_x).wait()
    pl.semaphore_wait(barrier, count)
    start_far(0, 0)
    start_far(0, 1)
    pack_half(0, FAR)
    start_far(0, 2)
    for per_layer in loads_w:
        for load in per_layer:
            load.start()
    for block in (0, 2, 1):
        pack_frames(0, block)
        send_frames(0, block)
    pack_half(0, NEAR)
    start_near(0, False)
    blank()
    for row in range(rows):
        put_row_upper(0, row)
    split_weights(0)
    seen = set()
    parts = parts_of(range(rows), seen)
    inner(0, parts, 0, 1, both[1:])
    start_near(0, True)
    take_frames(0, 0)
    each_piece(0, FAR, range(3, 5), "start")
    take_frames(0, 2)
    each_piece(0, NEAR, range(3, 5), "start")
    inner(0, parts, 1, 1, both[1:])
    forward(0, 0)
    inner(0, parts, 2, 1, both[1:])
    take_frames(0, 1)
    for row in range(rows):
        put_row_lower(0, row)
    parts = parts_of(range(rows), seen)
    forward(0, 1)
    inner(0, parts, 0, 2, both[:1])
    forward(0, 2)
    inner(0, parts, 2, 1, both[:1])
    for layer in range(layers):
        final = layer == layers - 1
        after = layer + 1
        for row in range(1, last):
            finish(layer, row)
        if not final:
            pack_frames(after, 1)
            drain_frames(layer, 1)
            send_frames(after, 1)
            split_weights(after)
        outer(layer, FAR)
        finish(layer, 0)
        if not final:
            each_piece(layer, FAR, range(5), "wait_send")
            start_far(after, 0)
            start_far(after, 1)
            pack_half(after, FAR)
            start_far(after, 2)
            pack_frames(after, 0)
            drain_frames(layer, 0)
            send_frames(after, 0)
        outer(layer, NEAR)
        if not final:
            finish(layer, last)
            each_piece(layer, NEAR, range(5), "wait_send")
            each_piece(after, NEAR, range(2), "start")
            pack_frames(after, 2)
            drain_frames(layer, 2)
            send_frames(after, 2)
            pack_half(after, NEAR)
            each_piece(after, NEAR, range(2, 3), "start")
            take_frames(after, 1)
            for row in range(1, last):
                put_row_upper(after, row)
                put_row_lower(after, row)
            seen = set()
            parts = parts_of(range(1, last), seen)
            inner(after, parts, 0, 2, both)
            for piece in range(3):

                @pl.when(relays(piece))
                def _():
                    relay_copy(layer, piece).wait_send()

            take_frames(after, 0)
            each_piece(after, FAR, range(3, 5), "start")
            forward(after, 0)
            inner(after, parts, 2, 1, both)
            take_frames(after, 2)
            each_piece(after, NEAR, range(3, 5), "start")
            forward(after, 1)
            put_row_upper(after, 0)
            put_row_lower(after, 0)
            inner(after, parts_of((0,), seen), 0, 3, both)
            forward(after, 2)
            put_row_upper(after, last)
            put_row_lower(after, last)
            inner(after, parts_of((last,), seen), 0, 3, both)

    drain(layers - 1)


def store(y_ref, w3, sx, acc, o_hbm, total, ready, sem):
    rows, cols, chans = y_ref.shape
    layers = w3.shape[0]
    last = rows - 1
    deep = 3 * LANES
    turned = lax.axis_index("row") % 2

    def place(row):
        return row + turned * (last - 2 * row)

    copies = [
        pltpu.make_async_copy(y_ref.at[place(row)], o_hbm.at[0, place(row)], sem.at[row]) for row in range(last)
    ]
    for copy in copies:
        copy.start()
    margin = jnp.zeros((3, PAD, chans), jnp.float32)
    total[:, pl.ds(0, PAD)] = margin
    total[:, pl.ds(PAD + cols, PAD)] = margin
    middle = cols // 2
    cuts = ((0, middle + 2 * PAD, 0, middle), (middle + 2 * PAD, cols, middle, cols))
    for n, (start, stop, begin, end) in enumerate(cuts):
        for tap in range(3):
            extra = jnp.dot(
                sx[rows + 1, pl.ds(start, stop - start), pl.ds(0, deep)],
                w3[layers - 1, tap, pl.ds(2 * deep, deep)],
                preferred_element_type=jnp.float32,
            )
            here = pl.ds(PAD + start, stop - start)
            total[tap, here] = acc[(layers - 1) % 2, tap, last, here] + extra
        size = end - begin
        value = total[0, pl.ds(PAD + begin - 1, size)] + total[1, pl.ds(PAD + begin, size)]
        ready[pl.ds(begin, size)] = jnp.maximum(value + total[2, pl.ds(PAD + begin + 1, size)], 0.0)
        copy = pltpu.make_async_copy(
            ready.at[pl.ds(begin, size)], o_hbm.at[0, place(last), pl.ds(begin, size)], sem.at[last + n]
        )
        copy.start()
        copies.append(copy)
    for copy in copies:
        copy.wait()


def local(features, conv_weight):
    _, rows, cols, chans = features.shape
    layers = conv_weight.shape[0]
    fold = chans // 8
    part = cols // (LANES // fold)
    halved = cols // (LANES // (LANES - 2 * fold))
    f32, bf16 = jnp.float32, jnp.bfloat16
    dma = pltpu.SemaphoreType.DMA
    results = pl.pallas_call(
        kernel,
        out_shape=(
            pltpu.VMEM((rows, cols, chans), f32),
            pltpu.VMEM((layers, 3, 9 * chans, chans), bf16),
            pltpu.VMEM((rows + 2, cols, 3 * chans), bf16),
            pltpu.VMEM((2, 3, rows, cols + 2 * PAD, chans), f32),
        ),
        in_specs=[pl.BlockSpec(memory_space=pl.ANY)] * 2,
        out_specs=(pl.BlockSpec(memory_space=pltpu.VMEM),) * 4,
        scratch_shapes=[
            pltpu.VMEM((rows, cols, chans), f32),
            pltpu.VMEM(conv_weight.shape, f32),
            pltpu.VMEM((layers - 1, rows, cols, chans), f32),
            pltpu.VMEM((layers, 2, rows, part, LANES), f32),
            pltpu.VMEM((layers, 2, rows, part, LANES), f32),
            pltpu.VMEM((layers, 2, halved, LANES), f32),
            pltpu.VMEM((layers, 2, cols, chans - LANES), f32),
            pltpu.VMEM((layers, 2, halved, LANES), f32),
            pltpu.VMEM((layers, 2, 2, part, LANES), f32),
            pltpu.VMEM((layers, cols, chans - LANES), f32),
            pltpu.VMEM((layers, halved, LANES), f32),
            dma,
            dma((layers,)),
            dma((2, 5)),
            dma((layers, 2, 5)),
            dma((2, 3)),
            dma((layers, 2, 3)),
            dma((3,)),
            dma((layers, 3)),
        ],
        compiler_params=pltpu.CompilerParams(
            collective_id=0, has_side_effects=True, vmem_limit_bytes=47 * 1024 * 1024
        ),
    )(features, conv_weight)
    return pl.pallas_call(
        store,
        out_shape=jax.ShapeDtypeStruct(features.shape, f32),
        in_specs=[pl.BlockSpec(memory_space=pltpu.VMEM)] * 4,
        out_specs=pl.BlockSpec(memory_space=pl.ANY),
        scratch_shapes=[
            pltpu.VMEM((3, cols + 2 * PAD, chans), f32),
            pltpu.VMEM((cols, chans), f32),
            dma((rows + 1,)),
        ],
        compiler_params=pltpu.CompilerParams(vmem_limit_bytes=4 * 1024 * 1024),
    )(*results)


def solution(mesh):
    placed = (P("frame", "row", None, None), P())
    return jax.shard_map(
        local, mesh=mesh, in_specs=placed, out_specs=P("frame", "row", None, None), check_vma=False
    )
```

```python
import jax
import jax.numpy as jnp
from jax import lax
from jax.experimental import pallas as pl
from jax.experimental.pallas import tpu as pltpu
from jax.sharding import PartitionSpec as P

MESH = pl.DeviceIdType.MESH
LANES = 128
PAD = 8
FAR, NEAR = 0, 1


def split(value):
    high = value.astype(jnp.bfloat16)
    low = (value - high.astype(jnp.float32)).astype(jnp.bfloat16)
    return high, low


def kernel(
    x_hbm, w_hbm, out, w3, sx, acc, xin, wbuf, mid, pack, got, half, hmain, hhalf, hshift, rmain, rhalf,
    load_x, load_w, row_send, row_recv, frame_send, frame_recv, relay_send, relay_recv,
):
    rows, cols, chans = xin.shape
    layers = wbuf.shape[0]
    tiles = chans // LANES
    both = range(tiles)
    fold = chans // 8
    last = rows - 1
    groups = LANES // fold
    part = cols // groups
    rest = LANES - 2 * fold
    halves = LANES // rest
    frames, bands = lax.axis_size("frame"), lax.axis_size("row")
    t, r = lax.axis_index("frame"), lax.axis_index("row")
    turned = r % 2
    sign = 1 - 2 * turned
    row_to = (r - sign, r + sign)
    has_row = tuple((peer >= 0) & (peer < bands) for peer in row_to)
    edge = (0, last)
    has_frame = (t > 0, t < frames - 1)
    frame_to = (t - 1, t + 1)

    pairs = bands // 2

    def shared(place):
        step = place // 2
        return 4 * (step + (place % 2) * (pairs - 1 - 2 * step)) // pairs

    def takes(place, piece):
        return shared(place) > piece

    def within(place):
        return (place >= 0) & (place < bands)

    def relayed(piece):
        return has_row[FAR] & has_row[NEAR] & takes(r, piece)

    onward = r + 2 * sign
    behind = r - 2 * sign

    def relays(piece):
        return has_row[NEAR] & within(onward) & takes(row_to[NEAR], piece)

    def place(row, count):
        return row + turned * (count - 1 - 2 * row)

    loads_x = [pltpu.make_async_copy(x_hbm.at[0, place(q, rows)], xin.at[q], load_x) for q in range(rows)]
    loads_w = [
        [pltpu.make_async_copy(w_hbm.at[n, place(d, 3)], wbuf.at[n, d], load_w.at[n]) for d in range(3)]
        for n in range(layers)
    ]
    for load in loads_x:
        load.start()

    barrier = pltpu.get_barrier_semaphore()
    count = 0
    for have, axis, peers in ((has_row, "row", row_to), (has_frame, "frame", frame_to)):
        for side in range(2):
            count = count + have[side].astype(jnp.int32)

            @pl.when(have[side])
            def _():
                pl.semaphore_signal(barrier, inc=1, device_id={axis: peers[side]}, device_id_type=MESH)

    for peer in (onward, behind):
        count = count + within(peer).astype(jnp.int32)

        @pl.when(within(peer))
        def _():
            pl.semaphore_signal(barrier, inc=1, device_id={"row": peer}, device_id_type=MESH)

    def maps(layer):
        return xin if layer == 0 else mid.at[layer - 1]

    def section(piece):
        return pl.ds(piece * (cols // 2), cols // 2)

    def row_copy(layer, kind, piece, relay=False):
        if piece < 2:
            source = maps(layer).at[edge[kind], section(piece), pl.ds(LANES, chans - LANES)]
            target = (rmain.at[layer] if relay else hmain.at[layer, kind]).at[section(piece)]
        elif piece == 2:
            source = half.at[layer, kind]
            target = rhalf.at[layer] if relay else hhalf.at[layer, kind]
        else:
            source = got.at[layer, piece - 3, edge[kind]]
            target = hshift.at[layer, kind, piece - 3]
        return pltpu.make_async_remote_copy(
            src_ref=source,
            dst_ref=target,
            send_sem=row_send.at[kind, piece],
            recv_sem=relay_recv.at[layer, piece] if relay else row_recv.at[layer, kind, piece],
            device_id={"row": row_to[NEAR if relay else kind]},
            device_id_type=MESH,
        )

    def relay_copy(layer, piece):
        if piece < 2:
            source, target = (ref.at[section(piece)] for ref in (rmain.at[layer], hmain.at[layer, FAR]))
        else:
            source, target = rhalf.at[layer], hhalf.at[layer, FAR]
        return pltpu.make_async_remote_copy(
            src_ref=source,
            dst_ref=target,
            send_sem=relay_send.at[piece],
            recv_sem=row_recv.at[layer, FAR, piece],
            device_id={"row": onward},
            device_id_type=MESH,
        )

    def start_far(layer, piece):
        @pl.when(relayed(piece))
        def _():
            row_copy(layer, FAR, piece, True).start()

        @pl.when(has_row[FAR] & jnp.logical_not(relayed(piece)))
        def _():
            row_copy(layer, FAR, piece).start()

    def drain_frames(layer, block):
        for side in range(2):

            @pl.when(has_frame[side])
            def _():
                frame_copy(layer, side, block).wait_send()

    def drain(layer):
        for kind in range(2):
            each_piece(layer, kind, range(5), "wait_send")
        for piece in range(3):

            @pl.when(relays(piece))
            def _():
                relay_copy(layer, piece).wait_send()

        for block in range(len(blocks)):
            drain_frames(layer, block)

    def start_near(layer, late):
        @pl.when(has_row[NEAR] & (relayed(1) if late else jnp.logical_not(relayed(1))))
        def _():
            for piece in range(3):
                row_copy(layer, NEAR, piece).start()

    def forward(layer, piece):
        @pl.when(relays(piece))
        def _():
            row_copy(layer, FAR, piece, True).wait_recv()
            relay_copy(layer, piece).start()

    def sent(kind, piece):
        return has_row[kind] if piece < 3 else has_row[kind] & has_frame[4 - piece]

    def each_piece(layer, kind, pieces, action):
        for piece in pieces:

            @pl.when(sent(kind, piece))
            def _():
                getattr(row_copy(layer, kind, piece), action)()

    blocks = ((0, 1), (1, rows - 2), (last, 1))

    def frame_copy(layer, side, block):
        start, size = blocks[block]
        return pltpu.make_async_remote_copy(
            src_ref=pack.at[layer, side, pl.ds(start, size)],
            dst_ref=got.at[layer, side, pl.ds(start, size)],
            send_sem=frame_send.at[side, block],
            recv_sem=frame_recv.at[layer, side, block],
            device_id={"frame": frame_to[side]},
            device_id_type=MESH,
        )

    def pack_frames(layer, block):
        start, size = blocks[block]
        lane = lax.broadcasted_iota(jnp.int32, (part, LANES), 1)
        for side in range(2):
            for row in range(start, start + size):
                full = None
                for group in range(groups):
                    value = maps(layer)[row, pl.ds(group * part, part), pl.ds(0, LANES)]
                    shift = ((group - side) * fold) % LANES
                    value = pltpu.roll(value, shift, 1) if shift else value
                    full = value if full is None else jnp.where(lane // fold == group, value, full)
                pack[layer, side, row] = full

    def send_frames(layer, block):
        for side in range(2):

            @pl.when(has_frame[side])
            def _():
                frame_copy(layer, side, block).start()

    def take_frames(layer, block):
        for side in range(2):

            @pl.when(has_frame[1 - side])
            def _():
                frame_copy(layer, side, block).wait_recv()

    def pack_half(layer, kind):
        size = cols // halves
        lane = lax.broadcasted_iota(jnp.int32, (size, LANES), 1)
        full = None
        for group in range(halves):
            value = maps(layer)[edge[kind], pl.ds(group * size, size), pl.ds(0, LANES)]
            shift = (group * rest - 2 * fold) % LANES
            value = pltpu.roll(value, shift, 1) if shift else value
            full = value if full is None else jnp.where(lane // rest == group, value, full)
        half[layer, kind] = full

    def put(spot, start, size, tile, value):
        high, low = split(value)
        for n, piece in enumerate((high, low, high)):
            sx[spot, pl.ds(start, size), pl.ds((3 * tile + n) * LANES, LANES)] = piece

    def put_upper(spot, source):
        for tile in range(1, tiles):
            put(spot, 0, cols, tile, source[:, pl.ds((tile - 1) * LANES, LANES)])

    def put_lower(spot, rest_of, shifted):
        lane = lax.broadcasted_iota(jnp.int32, (part, LANES), 1)
        for group in range(groups):
            value = rest_of(group * part)
            for side in range(2):
                moved = shifted(side)
                shift = ((side - group) * fold) % LANES
                moved = pltpu.roll(moved, shift, 1) if shift else moved
                value = jnp.where(lane // fold == side, moved, value)
            put(spot, group * part, part, 0, value)

    def put_row_upper(layer, row):
        put_upper(row + 1, maps(layer).at[row, :, pl.ds(LANES, chans - LANES)])

    def put_row_lower(layer, row):
        put_lower(
            row + 1,
            lambda start: maps(layer)[row, pl.ds(start, part), pl.ds(0, LANES)],
            lambda side: got[layer, side, row],
        )

    def put_halo(layer, kind):
        spot = 0 if kind == FAR else rows + 1
        size = cols // halves

        def rest_of(start):
            group = start // size
            value = hhalf[layer, kind, pl.ds(start - group * size, part)]
            shift = (2 * fold - group * rest) % LANES
            return pltpu.roll(value, shift, 1) if shift else value

        put_lower(spot, rest_of, lambda side: hshift[layer, kind, side])

    def split_weights(layer):
        pltpu.make_async_copy(w_hbm.at[layer], wbuf.at[layer], load_w.at[layer]).wait()

        def tap(index, carry):
            down, across = index // 3, index % 3
            high, low = split(wbuf[layer, down, across])
            for tile in range(tiles):
                span = slice(tile * LANES, (tile + 1) * LANES)
                base = pl.multiple_of((3 * tile + down) * 3 * LANES, LANES)
                for n, piece in enumerate((high, high, low)):
                    w3[layer, across, pl.ds(base + n * LANES, LANES)] = piece[span]
            return carry

        lax.fori_loop(0, 9, tap, 0)

    def parts_of(sources, seen):
        parts = []
        for row in range(rows):
            downs = [down for down in range(3) if row + down - 1 in sources]
            if downs:
                key = (downs[0], downs[-1] + 1, row in seen)
                if parts and parts[-1][2:] == key and sum(parts[-1][:2]) == row:
                    parts[-1] = (parts[-1][0], parts[-1][1] + 1) + key
                else:
                    parts.append((row, 1) + key)
        seen.update(part[0] + n for part in parts for n in range(part[1]))
        return parts

    def inner(layer, parts, first_tap, taps, which):
        deep = 3 * LANES

        def across(tap, carry):
            for first, count, low, high, add in parts:
                left = jnp.concatenate(
                    [
                        sx[pl.ds(first + down, count), :, pl.ds(tile * deep, deep)].reshape(count * cols, deep)
                        for tile in which
                        for down in range(low, high)
                    ],
                    axis=1,
                )
                right = jnp.concatenate(
                    [
                        w3[layer, tap, pl.ds((3 * tile + low) * deep, (high - low) * deep)]
                        for tile in which
                    ],
                    axis=0,
                )
                total = jnp.dot(left, right, preferred_element_type=jnp.float32)
                total = total.reshape(count, cols, chans)
                if add:
                    acc[layer % 2, tap, pl.ds(first, count), pl.ds(PAD, cols)] += total
                else:
                    acc[layer % 2, tap, pl.ds(first, count), pl.ds(PAD, cols)] = total
            return carry

        lax.fori_loop(first_tap, first_tap + taps, across, 0)

    def outer(layer, kind):
        spot = 0 if kind == FAR else rows + 1
        parts = ((0, 1, 0, 1, True),) if kind == FAR else ((last, 1, 2, 3, True),)
        steps = (both[1:], both[:1]) if layer == layers - 1 and kind == NEAR else (both,)
        for step in steps:

            @pl.when(has_row[kind])
            def _():
                if 1 in step:
                    each_piece(layer, kind, range(2), "wait_recv")
                    put_upper(spot, hmain.at[layer, kind])
                if 0 in step:
                    each_piece(layer, kind, range(2, 5), "wait_recv")
                    put_halo(layer, kind)

            if steps == (both,) or 0 not in step:
                inner(layer, parts, 0, 3, step)

    def finish(layer, row):
        part = acc.at[layer % 2, :, row]
        total = part[0, pl.ds(PAD - 1, cols)] + part[1, pl.ds(PAD, cols)]
        total = jnp.maximum(total + part[2, pl.ds(PAD + 1, cols)], 0.0)
        if layer == layers - 1:
            out[place(row, rows)] = total
        else:
            mid[layer, row] = total

    def blank():
        margin = jnp.zeros((2, 3, rows, PAD, chans), jnp.float32)
        acc[:, :, :, pl.ds(0, PAD)] = margin
        acc[:, :, :, pl.ds(PAD + cols, PAD)] = margin
        for kind, spot in ((FAR, 0), (NEAR, rows + 1)):

            @pl.when(jnp.logical_not(has_row[kind]))
            def _():
                sx[spot] = jnp.zeros((cols, 3 * chans), jnp.bfloat16)

        for side in range(2):

            @pl.when(jnp.logical_not(has_frame[1 - side]))
            def _():
                for layer in range(layers):
                    got[layer, side] = jnp.zeros((rows, part, LANES), jnp.float32)
                    for kind in range(2):
                        hshift[layer, kind, side] = jnp.zeros((part, LANES), jnp.float32)

    pltpu.make_async_copy(x_hbm.at[0], xin, load_x).wait()
    for per_layer in loads_w:
        for load in per_layer:
            load.start()
    pack_half(0, FAR)
    for block in (0, 2, 1):
        pack_frames(0, block)
    pack_half(0, NEAR)
    pl.semaphore_wait(barrier, count)
    send_frames(0, 0)
    send_frames(0, 2)
    for piece in range(3):
        start_far(0, piece)
    send_frames(0, 1)
    start_near(0, False)
    blank()
    for row in range(rows):
        put_row_upper(0, row)
    split_weights(0)
    seen = set()
    parts = parts_of(range(rows), seen)
    inner(0, parts, 0, 1, both[1:])
    start_near(0, True)
    take_frames(0, 0)
    each_piece(0, FAR, range(3, 5), "start")
    take_frames(0, 2)
    each_piece(0, NEAR, range(3, 5), "start")
    inner(0, parts, 1, 1, both[1:])
    forward(0, 0)
    inner(0, parts, 2, 1, both[1:])
    take_frames(0, 1)
    for row in range(rows):
        put_row_lower(0, row)
    parts = parts_of(range(rows), seen)
    forward(0, 1)
    inner(0, parts, 0, 2, both[:1])
    forward(0, 2)
    inner(0, parts, 2, 1, both[:1])
    for layer in range(layers):
        final = layer == layers - 1
        after = layer + 1
        for row in range(1, last):
            finish(layer, row)
        if not final:
            pack_frames(after, 1)
            drain_frames(layer, 1)
            send_frames(after, 1)
            split_weights(after)
        outer(layer, FAR)
        finish(layer, 0)
        if not final:
            each_piece(layer, FAR, range(5), "wait_send")
            start_far(after, 0)
            start_far(after, 1)
            pack_half(after, FAR)
            start_far(after, 2)
            pack_frames(after, 0)
            drain_frames(layer, 0)
            send_frames(after, 0)
        outer(layer, NEAR)
        if not final:
            finish(layer, last)
            each_piece(layer, NEAR, range(5), "wait_send")
            each_piece(after, NEAR, range(2), "start")
            pack_frames(after, 2)
            drain_frames(layer, 2)
            send_frames(after, 2)
            pack_half(after, NEAR)
            each_piece(after, NEAR, range(2, 3), "start")
            take_frames(after, 1)
            for row in range(1, last):
                put_row_upper(after, row)
                put_row_lower(after, row)
            seen = set()
            parts = parts_of(range(1, last), seen)
            inner(after, parts, 0, 2, both)
            for piece in range(3):

                @pl.when(relays(piece))
                def _():
                    relay_copy(layer, piece).wait_send()

            take_frames(after, 0)
            each_piece(after, FAR, range(3, 5), "start")
            forward(after, 0)
            inner(after, parts, 2, 1, both)
            take_frames(after, 2)
            each_piece(after, NEAR, range(3, 5), "start")
            forward(after, 1)
            put_row_upper(after, 0)
            put_row_lower(after, 0)
            inner(after, parts_of((0,), seen), 0, 3, both)
            forward(after, 2)
            put_row_upper(after, last)
            put_row_lower(after, last)
            inner(after, parts_of((last,), seen), 0, 3, both)

    drain(layers - 1)


def store(y_ref, w3, sx, acc, o_hbm, total, ready, sem):
    rows, cols, chans = y_ref.shape
    layers = w3.shape[0]
    last = rows - 1
    deep = 3 * LANES
    turned = lax.axis_index("row") % 2

    def place(row):
        return row + turned * (last - 2 * row)

    copies = [
        pltpu.make_async_copy(y_ref.at[place(row)], o_hbm.at[0, place(row)], sem.at[row]) for row in range(last)
    ]
    for copy in copies:
        copy.start()
    margin = jnp.zeros((3, PAD, chans), jnp.float32)
    total[:, pl.ds(0, PAD)] = margin
    total[:, pl.ds(PAD + cols, PAD)] = margin
    middle = cols // 2
    cuts = ((0, middle + 2 * PAD, 0, middle), (middle + 2 * PAD, cols, middle, cols))
    for n, (start, stop, begin, end) in enumerate(cuts):
        for tap in range(3):
            extra = jnp.dot(
                sx[rows + 1, pl.ds(start, stop - start), pl.ds(0, deep)],
                w3[layers - 1, tap, pl.ds(2 * deep, deep)],
                preferred_element_type=jnp.float32,
            )
            here = pl.ds(PAD + start, stop - start)
            total[tap, here] = acc[(layers - 1) % 2, tap, last, here] + extra
        size = end - begin
        value = total[0, pl.ds(PAD + begin - 1, size)] + total[1, pl.ds(PAD + begin, size)]
        ready[pl.ds(begin, size)] = jnp.maximum(value + total[2, pl.ds(PAD + begin + 1, size)], 0.0)
        copy = pltpu.make_async_copy(
            ready.at[pl.ds(begin, size)], o_hbm.at[0, place(last), pl.ds(begin, size)], sem.at[last + n]
        )
        copy.start()
        copies.append(copy)
    for copy in copies:
        copy.wait()


def local(features, conv_weight):
    _, rows, cols, chans = features.shape
    layers = conv_weight.shape[0]
    fold = chans // 8
    part = cols // (LANES // fold)
    halved = cols // (LANES // (LANES - 2 * fold))
    f32, bf16 = jnp.float32, jnp.bfloat16
    dma = pltpu.SemaphoreType.DMA
    results = pl.pallas_call(
        kernel,
        out_shape=(
            pltpu.VMEM((rows, cols, chans), f32),
            pltpu.VMEM((layers, 3, 9 * chans, chans), bf16),
            pltpu.VMEM((rows + 2, cols, 3 * chans), bf16),
            pltpu.VMEM((2, 3, rows, cols + 2 * PAD, chans), f32),
        ),
        in_specs=[pl.BlockSpec(memory_space=pl.ANY)] * 2,
        out_specs=(pl.BlockSpec(memory_space=pltpu.VMEM),) * 4,
        scratch_shapes=[
            pltpu.VMEM((rows, cols, chans), f32),
            pltpu.VMEM(conv_weight.shape, f32),
            pltpu.VMEM((layers - 1, rows, cols, chans), f32),
            pltpu.VMEM((layers, 2, rows, part, LANES), f32),
            pltpu.VMEM((layers, 2, rows, part, LANES), f32),
            pltpu.VMEM((layers, 2, halved, LANES), f32),
            pltpu.VMEM((layers, 2, cols, chans - LANES), f32),
            pltpu.VMEM((layers, 2, halved, LANES), f32),
            pltpu.VMEM((layers, 2, 2, part, LANES), f32),
            pltpu.VMEM((layers, cols, chans - LANES), f32),
            pltpu.VMEM((layers, halved, LANES), f32),
            dma,
            dma((layers,)),
            dma((2, 5)),
            dma((layers, 2, 5)),
            dma((2, 3)),
            dma((layers, 2, 3)),
            dma((3,)),
            dma((layers, 3)),
        ],
        compiler_params=pltpu.CompilerParams(
            collective_id=0, has_side_effects=True, vmem_limit_bytes=47 * 1024 * 1024
        ),
    )(features, conv_weight)
    return pl.pallas_call(
        store,
        out_shape=jax.ShapeDtypeStruct(features.shape, f32),
        in_specs=[pl.BlockSpec(memory_space=pltpu.VMEM)] * 4,
        out_specs=pl.BlockSpec(memory_space=pl.ANY),
        scratch_shapes=[
            pltpu.VMEM((3, cols + 2 * PAD, chans), f32),
            pltpu.VMEM((cols, chans), f32),
            dma((rows + 1,)),
        ],
        compiler_params=pltpu.CompilerParams(vmem_limit_bytes=4 * 1024 * 1024),
    )(*results)


def solution(mesh):
    placed = (P("frame", "row", None, None), P())
    return jax.shard_map(
        local, mesh=mesh, in_specs=placed, out_specs=P("frame", "row", None, None), check_vma=False
    )
```

```python
import jax
import jax.numpy as jnp
from jax import lax
from jax.experimental import pallas as pl
from jax.experimental.pallas import tpu as pltpu
from jax.sharding import PartitionSpec as P

MESH = pl.DeviceIdType.MESH
LANES = 128
PAD = 8
FAR, NEAR = 0, 1


def split(value):
    high = value.astype(jnp.bfloat16)
    low = (value - high.astype(jnp.float32)).astype(jnp.bfloat16)
    return high, low


def kernel(
    x_hbm, w_hbm, out, w3, sx, acc, xin, wbuf, mid, pack, got, half, hmain, hhalf, hshift, rmain, rhalf,
    load_x, load_w, row_send, row_recv, frame_send, frame_recv, relay_send, relay_recv,
):
    rows, cols, chans = xin.shape
    layers = wbuf.shape[0]
    tiles = chans // LANES
    both = range(tiles)
    fold = chans // 8
    last = rows - 1
    groups = LANES // fold
    part = cols // groups
    rest = LANES - 2 * fold
    halves = LANES // rest
    frames, bands = lax.axis_size("frame"), lax.axis_size("row")
    t, r = lax.axis_index("frame"), lax.axis_index("row")
    turned = r % 2
    sign = 1 - 2 * turned
    row_to = (r - sign, r + sign)
    has_row = tuple((peer >= 0) & (peer < bands) for peer in row_to)
    edge = (0, last)
    has_frame = (t > 0, t < frames - 1)
    frame_to = (t - 1, t + 1)

    pairs = bands // 2

    def shared(place):
        step = place // 2
        return 4 * (step + (place % 2) * (pairs - 1 - 2 * step)) // pairs

    def takes(place, piece):
        return shared(place) > piece

    def within(place):
        return (place >= 0) & (place < bands)

    def relayed(piece):
        return has_row[FAR] & has_row[NEAR] & takes(r, piece)

    onward = r + 2 * sign
    behind = r - 2 * sign

    def relays(piece):
        return has_row[NEAR] & within(onward) & takes(row_to[NEAR], piece)

    def place(row, count):
        return row + turned * (count - 1 - 2 * row)

    loads_x = [pltpu.make_async_copy(x_hbm.at[0, place(q, rows)], xin.at[q], load_x) for q in range(rows)]
    loads_w = [
        [pltpu.make_async_copy(w_hbm.at[n, place(d, 3)], wbuf.at[n, d], load_w.at[n]) for d in range(3)]
        for n in range(layers)
    ]
    for load in loads_x:
        load.start()

    barrier = pltpu.get_barrier_semaphore()
    count = 0
    for have, axis, peers in ((has_row, "row", row_to), (has_frame, "frame", frame_to)):
        for side in range(2):
            count = count + have[side].astype(jnp.int32)

            @pl.when(have[side])
            def _():
                pl.semaphore_signal(barrier, inc=1, device_id={axis: peers[side]}, device_id_type=MESH)

    for peer in (onward, behind):
        count = count + within(peer).astype(jnp.int32)

        @pl.when(within(peer))
        def _():
            pl.semaphore_signal(barrier, inc=1, device_id={"row": peer}, device_id_type=MESH)

    def maps(layer):
        return xin if layer == 0 else mid.at[layer - 1]

    def section(piece):
        return pl.ds(piece * (cols // 2), cols // 2)

    def row_copy(layer, kind, piece, relay=False):
        if piece < 2:
            source = maps(layer).at[edge[kind], section(piece), pl.ds(LANES, chans - LANES)]
            target = (rmain.at[layer] if relay else hmain.at[layer, kind]).at[section(piece)]
        elif piece == 2:
            source = half.at[layer, kind]
            target = rhalf.at[layer] if relay else hhalf.at[layer, kind]
        else:
            source = got.at[layer, piece - 3, edge[kind]]
            target = hshift.at[layer, kind, piece - 3]
        return pltpu.make_async_remote_copy(
            src_ref=source,
            dst_ref=target,
            send_sem=row_send.at[kind, piece],
            recv_sem=relay_recv.at[layer, piece] if relay else row_recv.at[layer, kind, piece],
            device_id={"row": row_to[NEAR if relay else kind]},
            device_id_type=MESH,
        )

    def relay_copy(layer, piece):
        if piece < 2:
            source, target = (ref.at[section(piece)] for ref in (rmain.at[layer], hmain.at[layer, FAR]))
        else:
            source, target = rhalf.at[layer], hhalf.at[layer, FAR]
        return pltpu.make_async_remote_copy(
            src_ref=source,
            dst_ref=target,
            send_sem=relay_send.at[piece],
            recv_sem=row_recv.at[layer, FAR, piece],
            device_id={"row": onward},
            device_id_type=MESH,
        )

    def start_far(layer, piece):
        @pl.when(relayed(piece))
        def _():
            row_copy(layer, FAR, piece, True).start()

        @pl.when(has_row[FAR] & jnp.logical_not(relayed(piece)))
        def _():
            row_copy(layer, FAR, piece).start()

    def drain_frames(layer, block):
        for side in range(2):

            @pl.when(has_frame[side])
            def _():
                frame_copy(layer, side, block).wait_send()

    def drain(layer):
        for kind in range(2):
            each_piece(layer, kind, range(5), "wait_send")
        for piece in range(3):

            @pl.when(relays(piece))
            def _():
                relay_copy(layer, piece).wait_send()

        for block in range(len(blocks)):
            drain_frames(layer, block)

    def start_near(layer, late):
        @pl.when(has_row[NEAR] & (relayed(1) if late else jnp.logical_not(relayed(1))))
        def _():
            for piece in range(3):
                row_copy(layer, NEAR, piece).start()

    def forward(layer, piece):
        @pl.when(relays(piece))
        def _():
            row_copy(layer, FAR, piece, True).wait_recv()
            relay_copy(layer, piece).start()

    def sent(kind, piece):
        return has_row[kind] if piece < 3 else has_row[kind] & has_frame[4 - piece]

    prompt = has_row[FAR] & (shared(row_to[FAR]) <= 1)

    def each_piece(layer, kind, pieces, action):
        for piece in pieces:

            @pl.when(sent(kind, piece))
            def _():
                getattr(row_copy(layer, kind, piece), action)()

    blocks = ((0, 1), (1, rows - 2), (last, 1))

    def frame_copy(layer, side, block):
        start, size = blocks[block]
        return pltpu.make_async_remote_copy(
            src_ref=pack.at[layer, side, pl.ds(start, size)],
            dst_ref=got.at[layer, side, pl.ds(start, size)],
            send_sem=frame_send.at[side, block],
            recv_sem=frame_recv.at[layer, side, block],
            device_id={"frame": frame_to[side]},
            device_id_type=MESH,
        )

    def pack_frames(layer, block):
        start, size = blocks[block]
        lane = lax.broadcasted_iota(jnp.int32, (part, LANES), 1)
        for side in range(2):
            for row in range(start, start + size):
                full = None
                for group in range(groups):
                    value = maps(layer)[row, pl.ds(group * part, part), pl.ds(0, LANES)]
                    shift = ((group - side) * fold) % LANES
                    value = pltpu.roll(value, shift, 1) if shift else value
                    full = value if full is None else jnp.where(lane // fold == group, value, full)
                pack[layer, side, row] = full

    def send_frames(layer, block):
        for side in range(2):

            @pl.when(has_frame[side])
            def _():
                frame_copy(layer, side, block).start()

    def take_frames(layer, block):
        for side in range(2):

            @pl.when(has_frame[1 - side])
            def _():
                frame_copy(layer, side, block).wait_recv()

    def pack_half(layer, kind):
        size = cols // halves
        lane = lax.broadcasted_iota(jnp.int32, (size, LANES), 1)
        full = None
        for group in range(halves):
            value = maps(layer)[edge[kind], pl.ds(group * size, size), pl.ds(0, LANES)]
            shift = (group * rest - 2 * fold) % LANES
            value = pltpu.roll(value, shift, 1) if shift else value
            full = value if full is None else jnp.where(lane // rest == group, value, full)
        half[layer, kind] = full

    def put(spot, start, size, tile, value):
        high, low = split(value)
        for n, piece in enumerate((high, low, high)):
            sx[spot, pl.ds(start, size), pl.ds((3 * tile + n) * LANES, LANES)] = piece

    def put_upper(spot, source):
        for tile in range(1, tiles):
            put(spot, 0, cols, tile, source[:, pl.ds((tile - 1) * LANES, LANES)])

    def put_lower(spot, rest_of, shifted):
        lane = lax.broadcasted_iota(jnp.int32, (part, LANES), 1)
        for group in range(groups):
            value = rest_of(group * part)
            for side in range(2):
                moved = shifted(side)
                shift = ((side - group) * fold) % LANES
                moved = pltpu.roll(moved, shift, 1) if shift else moved
                value = jnp.where(lane // fold == side, moved, value)
            put(spot, group * part, part, 0, value)

    def put_row_upper(layer, row):
        put_upper(row + 1, maps(layer).at[row, :, pl.ds(LANES, chans - LANES)])

    def put_row_lower(layer, row):
        put_lower(
            row + 1,
            lambda start: maps(layer)[row, pl.ds(start, part), pl.ds(0, LANES)],
            lambda side: got[layer, side, row],
        )

    def put_halo(layer, kind):
        spot = 0 if kind == FAR else rows + 1
        size = cols // halves

        def rest_of(start):
            group = start // size
            value = hhalf[layer, kind, pl.ds(start - group * size, part)]
            shift = (2 * fold - group * rest) % LANES
            return pltpu.roll(value, shift, 1) if shift else value

        put_lower(spot, rest_of, lambda side: hshift[layer, kind, side])

    def split_weights(layer):
        pltpu.make_async_copy(w_hbm.at[layer], wbuf.at[layer], load_w.at[layer]).wait()

        def tap(index, carry):
            down, across = index // 3, index % 3
            high, low = split(wbuf[layer, down, across])
            for tile in range(tiles):
                span = slice(tile * LANES, (tile + 1) * LANES)
                base = pl.multiple_of((3 * tile + down) * 3 * LANES, LANES)
                for n, piece in enumerate((high, high, low)):
                    w3[layer, across, pl.ds(base + n * LANES, LANES)] = piece[span]
            return carry

        lax.fori_loop(0, 9, tap, 0)

    def parts_of(sources, seen):
        parts = []
        for row in range(rows):
            downs = [down for down in range(3) if row + down - 1 in sources]
            if downs:
                key = (downs[0], downs[-1] + 1, row in seen)
                if parts and parts[-1][2:] == key and sum(parts[-1][:2]) == row:
                    parts[-1] = (parts[-1][0], parts[-1][1] + 1) + key
                else:
                    parts.append((row, 1) + key)
        seen.update(part[0] + n for part in parts for n in range(part[1]))
        return parts

    def inner(layer, parts, first_tap, taps, which):
        deep = 3 * LANES

        def across(tap, carry):
            for first, count, low, high, add in parts:
                left = jnp.concatenate(
                    [
                        sx[pl.ds(first + down, count), :, pl.ds(tile * deep, deep)].reshape(count * cols, deep)
                        for tile in which
                        for down in range(low, high)
                    ],
                    axis=1,
                )
                right = jnp.concatenate(
                    [
                        w3[layer, tap, pl.ds((3 * tile + low) * deep, (high - low) * deep)]
                        for tile in which
                    ],
                    axis=0,
                )
                total = jnp.dot(left, right, preferred_element_type=jnp.float32)
                total = total.reshape(count, cols, chans)
                if add:
                    acc[layer % 2, tap, pl.ds(first, count), pl.ds(PAD, cols)] += total
                else:
                    acc[layer % 2, tap, pl.ds(first, count), pl.ds(PAD, cols)] = total
            return carry

        lax.fori_loop(first_tap, first_tap + taps, across, 0)

    def outer(layer, kind):
        spot = 0 if kind == FAR else rows + 1
        parts = ((0, 1, 0, 1, True),) if kind == FAR else ((last, 1, 2, 3, True),)
        steps = (both[1:], both[:1]) if layer == layers - 1 and kind == NEAR else (both,)
        for step in steps:

            @pl.when(has_row[kind])
            def _():
                if 1 in step:
                    each_piece(layer, kind, range(2), "wait_recv")
                    put_upper(spot, hmain.at[layer, kind])
                if 0 in step:
                    each_piece(layer, kind, range(2, 5), "wait_recv")
                    put_halo(layer, kind)

            if steps == (both,) or 0 not in step:
                inner(layer, parts, 0, 3, step)

    def finish(layer, row):
        part = acc.at[layer % 2, :, row]
        total = part[0, pl.ds(PAD - 1, cols)] + part[1, pl.ds(PAD, cols)]
        total = jnp.maximum(total + part[2, pl.ds(PAD + 1, cols)], 0.0)
        if layer == layers - 1:
            out[place(row, rows)] = total
        else:
            mid[layer, row] = total

    def blank():
        margin = jnp.zeros((2, 3, rows, PAD, chans), jnp.float32)
        acc[:, :, :, pl.ds(0, PAD)] = margin
        acc[:, :, :, pl.ds(PAD + cols, PAD)] = margin
        for kind, spot in ((FAR, 0), (NEAR, rows + 1)):

            @pl.when(jnp.logical_not(has_row[kind]))
            def _():
                sx[spot] = jnp.zeros((cols, 3 * chans), jnp.bfloat16)

        for side in range(2):

            @pl.when(jnp.logical_not(has_frame[1 - side]))
            def _():
                for layer in range(layers):
                    got[layer, side] = jnp.zeros((rows, part, LANES), jnp.float32)
                    for kind in range(2):
                        hshift[layer, kind, side] = jnp.zeros((part, LANES), jnp.float32)

    pltpu.make_async_copy(x_hbm.at[0], xin, load_x).wait()
    for per_layer in loads_w:
        for load in per_layer:
            load.start()
    pack_half(0, FAR)
    for block in (0, 2, 1):
        pack_frames(0, block)
    pack_half(0, NEAR)
    pl.semaphore_wait(barrier, count)
    send_frames(0, 0)
    send_frames(0, 2)
    for piece in range(3):
        start_far(0, piece)
    send_frames(0, 1)
    start_near(0, False)
    blank()
    for row in range(rows):
        put_row_upper(0, row)
    split_weights(0)
    seen = set()
    parts = parts_of(range(rows), seen)
    inner(0, parts, 0, 1, both[1:])
    start_near(0, True)
    take_frames(0, 0)
    each_piece(0, FAR, range(3, 5), "start")
    take_frames(0, 2)
    each_piece(0, NEAR, range(3, 5), "start")
    inner(0, parts, 1, 1, both[1:])
    forward(0, 0)
    inner(0, parts, 2, 1, both[1:])
    take_frames(0, 1)
    for row in range(rows):
        put_row_lower(0, row)
    parts = parts_of(range(rows), seen)
    forward(0, 1)
    inner(0, parts, 0, 2, both[:1])
    forward(0, 2)
    inner(0, parts, 2, 1, both[:1])
    for layer in range(layers):
        final = layer == layers - 1
        after = layer + 1
        for row in range(1, last):
            finish(layer, row)
        if not final:
            pack_frames(after, 1)
            drain_frames(layer, 1)
            send_frames(after, 1)

            @pl.when(jnp.logical_not(prompt))
            def _():
                split_weights(after)

        outer(layer, FAR)
        finish(layer, 0)
        if not final:
            each_piece(layer, FAR, range(5), "wait_send")
            start_far(after, 0)
            start_far(after, 1)
            pack_half(after, FAR)
            start_far(after, 2)
            pack_frames(after, 0)
            drain_frames(layer, 0)
            send_frames(after, 0)

            @pl.when(prompt)
            def _():
                split_weights(after)

        outer(layer, NEAR)
        if not final:
            finish(layer, last)
            each_piece(layer, NEAR, range(5), "wait_send")
            each_piece(after, NEAR, range(2), "start")
            pack_frames(after, 2)
            drain_frames(layer, 2)
            send_frames(after, 2)
            pack_half(after, NEAR)
            each_piece(after, NEAR, range(2, 3), "start")
            take_frames(after, 1)
            for row in range(1, last):
                put_row_upper(after, row)
                put_row_lower(after, row)
            seen = set()
            parts = parts_of(range(1, last), seen)
            inner(after, parts, 0, 2, both)
            for piece in range(3):

                @pl.when(relays(piece))
                def _():
                    relay_copy(layer, piece).wait_send()

            take_frames(after, 0)
            each_piece(after, FAR, range(3, 5), "start")
            forward(after, 0)
            inner(after, parts, 2, 1, both)
            take_frames(after, 2)
            each_piece(after, NEAR, range(3, 5), "start")
            forward(after, 1)
            put_row_upper(after, 0)
            put_row_lower(after, 0)
            inner(after, parts_of((0,), seen), 0, 3, both)
            forward(after, 2)
            put_row_upper(after, last)
            put_row_lower(after, last)
            inner(after, parts_of((last,), seen), 0, 3, both)

    drain(layers - 1)


def store(y_ref, w3, sx, acc, o_hbm, total, ready, sem):
    rows, cols, chans = y_ref.shape
    layers = w3.shape[0]
    last = rows - 1
    deep = 3 * LANES
    turned = lax.axis_index("row") % 2

    def place(row):
        return row + turned * (last - 2 * row)

    copies = [
        pltpu.make_async_copy(y_ref.at[place(row)], o_hbm.at[0, place(row)], sem.at[row]) for row in range(last)
    ]
    for copy in copies:
        copy.start()
    margin = jnp.zeros((3, PAD, chans), jnp.float32)
    total[:, pl.ds(0, PAD)] = margin
    total[:, pl.ds(PAD + cols, PAD)] = margin
    middle = cols // 2
    cuts = ((0, middle + 2 * PAD, 0, middle), (middle + 2 * PAD, cols, middle, cols))
    for n, (start, stop, begin, end) in enumerate(cuts):
        for tap in range(3):
            extra = jnp.dot(
                sx[rows + 1, pl.ds(start, stop - start), pl.ds(0, deep)],
                w3[layers - 1, tap, pl.ds(2 * deep, deep)],
                preferred_element_type=jnp.float32,
            )
            here = pl.ds(PAD + start, stop - start)
            total[tap, here] = acc[(layers - 1) % 2, tap, last, here] + extra
        size = end - begin
        value = total[0, pl.ds(PAD + begin - 1, size)] + total[1, pl.ds(PAD + begin, size)]
        ready[pl.ds(begin, size)] = jnp.maximum(value + total[2, pl.ds(PAD + begin + 1, size)], 0.0)
        copy = pltpu.make_async_copy(
            ready.at[pl.ds(begin, size)], o_hbm.at[0, place(last), pl.ds(begin, size)], sem.at[last + n]
        )
        copy.start()
        copies.append(copy)
    for copy in copies:
        copy.wait()


def local(features, conv_weight):
    _, rows, cols, chans = features.shape
    layers = conv_weight.shape[0]
    fold = chans // 8
    part = cols // (LANES // fold)
    halved = cols // (LANES // (LANES - 2 * fold))
    f32, bf16 = jnp.float32, jnp.bfloat16
    dma = pltpu.SemaphoreType.DMA
    results = pl.pallas_call(
        kernel,
        out_shape=(
            pltpu.VMEM((rows, cols, chans), f32),
            pltpu.VMEM((layers, 3, 9 * chans, chans), bf16),
            pltpu.VMEM((rows + 2, cols, 3 * chans), bf16),
            pltpu.VMEM((2, 3, rows, cols + 2 * PAD, chans), f32),
        ),
        in_specs=[pl.BlockSpec(memory_space=pl.ANY)] * 2,
        out_specs=(pl.BlockSpec(memory_space=pltpu.VMEM),) * 4,
        scratch_shapes=[
            pltpu.VMEM((rows, cols, chans), f32),
            pltpu.VMEM(conv_weight.shape, f32),
            pltpu.VMEM((layers - 1, rows, cols, chans), f32),
            pltpu.VMEM((layers, 2, rows, part, LANES), f32),
            pltpu.VMEM((layers, 2, rows, part, LANES), f32),
            pltpu.VMEM((layers, 2, halved, LANES), f32),
            pltpu.VMEM((layers, 2, cols, chans - LANES), f32),
            pltpu.VMEM((layers, 2, halved, LANES), f32),
            pltpu.VMEM((layers, 2, 2, part, LANES), f32),
            pltpu.VMEM((layers, cols, chans - LANES), f32),
            pltpu.VMEM((layers, halved, LANES), f32),
            dma,
            dma((layers,)),
            dma((2, 5)),
            dma((layers, 2, 5)),
            dma((2, 3)),
            dma((layers, 2, 3)),
            dma((3,)),
            dma((layers, 3)),
        ],
        compiler_params=pltpu.CompilerParams(
            collective_id=0, has_side_effects=True, vmem_limit_bytes=47 * 1024 * 1024
        ),
    )(features, conv_weight)
    return pl.pallas_call(
        store,
        out_shape=jax.ShapeDtypeStruct(features.shape, f32),
        in_specs=[pl.BlockSpec(memory_space=pltpu.VMEM)] * 4,
        out_specs=pl.BlockSpec(memory_space=pl.ANY),
        scratch_shapes=[
            pltpu.VMEM((3, cols + 2 * PAD, chans), f32),
            pltpu.VMEM((cols, chans), f32),
            dma((rows + 1,)),
        ],
        compiler_params=pltpu.CompilerParams(vmem_limit_bytes=4 * 1024 * 1024),
    )(*results)


def solution(mesh):
    placed = (P("frame", "row", None, None), P())
    return jax.shard_map(
        local, mesh=mesh, in_specs=placed, out_specs=P("frame", "row", None, None), check_vma=False
    )
```

```python
import jax
import jax.numpy as jnp
from jax import lax
from jax.experimental import pallas as pl
from jax.experimental.pallas import tpu as pltpu
from jax.sharding import PartitionSpec as P

MESH = pl.DeviceIdType.MESH
LANES = 128
PAD = 8
FAR, NEAR = 0, 1


def split(value):
    high = value.astype(jnp.bfloat16)
    low = (value - high.astype(jnp.float32)).astype(jnp.bfloat16)
    return high, low


def kernel(
    x_hbm, w_hbm, out, w3, sx, acc, xin, wbuf, mid, pack, got, half, hmain, hhalf, hshift, rmain, rhalf,
    load_x, load_w, row_send, row_recv, frame_send, frame_recv, relay_send, relay_recv,
):
    rows, cols, chans = xin.shape
    layers = wbuf.shape[0]
    tiles = chans // LANES
    both = range(tiles)
    fold = chans // 8
    last = rows - 1
    groups = LANES // fold
    part = cols // groups
    rest = LANES - 2 * fold
    halves = LANES // rest
    frames, bands = lax.axis_size("frame"), lax.axis_size("row")
    t, r = lax.axis_index("frame"), lax.axis_index("row")
    turned = r % 2
    sign = 1 - 2 * turned
    row_to = (r - sign, r + sign)
    has_row = tuple((peer >= 0) & (peer < bands) for peer in row_to)
    edge = (0, last)
    has_frame = (t > 0, t < frames - 1)
    frame_to = (t - 1, t + 1)

    pairs = bands // 2

    def shared(place):
        step = place // 2
        return 4 * (step + (place % 2) * (pairs - 1 - 2 * step)) // pairs

    def takes(place, piece):
        return shared(place) > piece

    def within(place):
        return (place >= 0) & (place < bands)

    def relayed(piece):
        return has_row[FAR] & has_row[NEAR] & takes(r, piece)

    onward = r + 2 * sign
    behind = r - 2 * sign

    def relays(piece):
        return has_row[NEAR] & within(onward) & takes(row_to[NEAR], piece)

    def place(row, count):
        return row + turned * (count - 1 - 2 * row)

    loads_x = [pltpu.make_async_copy(x_hbm.at[0, place(q, rows)], xin.at[q], load_x) for q in range(rows)]
    loads_w = [
        [pltpu.make_async_copy(w_hbm.at[n, place(d, 3)], wbuf.at[n, d], load_w.at[n]) for d in range(3)]
        for n in range(layers)
    ]
    for load in loads_x:
        load.start()

    barrier = pltpu.get_barrier_semaphore()
    count = 0
    for have, axis, peers in ((has_row, "row", row_to), (has_frame, "frame", frame_to)):
        for side in range(2):
            count = count + have[side].astype(jnp.int32)

            @pl.when(have[side])
            def _():
                pl.semaphore_signal(barrier, inc=1, device_id={axis: peers[side]}, device_id_type=MESH)

    for peer in (onward, behind):
        count = count + within(peer).astype(jnp.int32)

        @pl.when(within(peer))
        def _():
            pl.semaphore_signal(barrier, inc=1, device_id={"row": peer}, device_id_type=MESH)

    def maps(layer):
        return xin if layer == 0 else mid.at[layer - 1]

    def section(piece):
        return pl.ds(piece * (cols // 2), cols // 2)

    def row_copy(layer, kind, piece, relay=False):
        if piece < 2:
            source = maps(layer).at[edge[kind], section(piece), pl.ds(LANES, chans - LANES)]
            target = (rmain.at[layer] if relay else hmain.at[layer, kind]).at[section(piece)]
        elif piece == 2:
            source = half.at[layer, kind]
            target = rhalf.at[layer] if relay else hhalf.at[layer, kind]
        else:
            source = got.at[layer, piece - 3, edge[kind]]
            target = hshift.at[layer, kind, piece - 3]
        return pltpu.make_async_remote_copy(
            src_ref=source,
            dst_ref=target,
            send_sem=row_send.at[kind, piece],
            recv_sem=relay_recv.at[layer, piece] if relay else row_recv.at[layer, kind, piece],
            device_id={"row": row_to[NEAR if relay else kind]},
            device_id_type=MESH,
        )

    def relay_copy(layer, piece):
        if piece < 2:
            source, target = (ref.at[section(piece)] for ref in (rmain.at[layer], hmain.at[layer, FAR]))
        else:
            source, target = rhalf.at[layer], hhalf.at[layer, FAR]
        return pltpu.make_async_remote_copy(
            src_ref=source,
            dst_ref=target,
            send_sem=relay_send.at[piece],
            recv_sem=row_recv.at[layer, FAR, piece],
            device_id={"row": onward},
            device_id_type=MESH,
        )

    def start_far(layer, piece):
        @pl.when(relayed(piece))
        def _():
            row_copy(layer, FAR, piece, True).start()

        @pl.when(has_row[FAR] & jnp.logical_not(relayed(piece)))
        def _():
            row_copy(layer, FAR, piece).start()

    def drain_frames(layer, block):
        for side in range(2):

            @pl.when(has_frame[side])
            def _():
                frame_copy(layer, side, block).wait_send()

    def drain(layer):
        for kind in range(2):
            each_piece(layer, kind, range(5), "wait_send")
        for piece in range(3):

            @pl.when(relays(piece))
            def _():
                relay_copy(layer, piece).wait_send()

        for block in range(len(blocks)):
            drain_frames(layer, block)

    def start_near(layer, late):
        @pl.when(has_row[NEAR] & (relayed(1) if late else jnp.logical_not(relayed(1))))
        def _():
            for piece in range(3):
                row_copy(layer, NEAR, piece).start()

    def forward(layer, piece):
        @pl.when(relays(piece))
        def _():
            row_copy(layer, FAR, piece, True).wait_recv()
            relay_copy(layer, piece).start()

    def sent(kind, piece):
        return has_row[kind] if piece < 3 else has_row[kind] & has_frame[4 - piece]

    prompt = has_row[FAR] & (shared(row_to[FAR]) <= 1)

    def each_piece(layer, kind, pieces, action):
        for piece in pieces:

            @pl.when(sent(kind, piece))
            def _():
                getattr(row_copy(layer, kind, piece), action)()

    blocks = ((0, 1), (1, rows - 2), (last, 1))

    def frame_copy(layer, side, block):
        start, size = blocks[block]
        return pltpu.make_async_remote_copy(
            src_ref=pack.at[layer, side, pl.ds(start, size)],
            dst_ref=got.at[layer, side, pl.ds(start, size)],
            send_sem=frame_send.at[side, block],
            recv_sem=frame_recv.at[layer, side, block],
            device_id={"frame": frame_to[side]},
            device_id_type=MESH,
        )

    def pack_frames(layer, block):
        start, size = blocks[block]
        lane = lax.broadcasted_iota(jnp.int32, (part, LANES), 1)
        for side in range(2):
            for row in range(start, start + size):
                full = None
                for group in range(groups):
                    value = maps(layer)[row, pl.ds(group * part, part), pl.ds(0, LANES)]
                    shift = ((group - side) * fold) % LANES
                    value = pltpu.roll(value, shift, 1) if shift else value
                    full = value if full is None else jnp.where(lane // fold == group, value, full)
                pack[layer, side, row] = full

    def send_frames(layer, block):
        for side in range(2):

            @pl.when(has_frame[side])
            def _():
                frame_copy(layer, side, block).start()

    def take_frames(layer, block):
        for side in range(2):

            @pl.when(has_frame[1 - side])
            def _():
                frame_copy(layer, side, block).wait_recv()

    def pack_half(layer, kind):
        size = cols // halves
        lane = lax.broadcasted_iota(jnp.int32, (size, LANES), 1)
        full = None
        for group in range(halves):
            value = maps(layer)[edge[kind], pl.ds(group * size, size), pl.ds(0, LANES)]
            shift = (group * rest - 2 * fold) % LANES
            value = pltpu.roll(value, shift, 1) if shift else value
            full = value if full is None else jnp.where(lane // rest == group, value, full)
        half[layer, kind] = full

    def put(spot, start, size, tile, value):
        high, low = split(value)
        for n, piece in enumerate((high, low, high)):
            sx[spot, pl.ds(start, size), pl.ds((3 * tile + n) * LANES, LANES)] = piece

    def put_upper(spot, source):
        for tile in range(1, tiles):
            put(spot, 0, cols, tile, source[:, pl.ds((tile - 1) * LANES, LANES)])

    def put_lower(spot, rest_of, shifted):
        lane = lax.broadcasted_iota(jnp.int32, (part, LANES), 1)
        for group in range(groups):
            value = rest_of(group * part)
            for side in range(2):
                moved = shifted(side)
                shift = ((side - group) * fold) % LANES
                moved = pltpu.roll(moved, shift, 1) if shift else moved
                value = jnp.where(lane // fold == side, moved, value)
            put(spot, group * part, part, 0, value)

    def put_row_upper(layer, row):
        put_upper(row + 1, maps(layer).at[row, :, pl.ds(LANES, chans - LANES)])

    def put_row_lower(layer, row):
        put_lower(
            row + 1,
            lambda start: maps(layer)[row, pl.ds(start, part), pl.ds(0, LANES)],
            lambda side: got[layer, side, row],
        )

    def put_halo(layer, kind):
        spot = 0 if kind == FAR else rows + 1
        size = cols // halves

        def rest_of(start):
            group = start // size
            value = hhalf[layer, kind, pl.ds(start - group * size, part)]
            shift = (2 * fold - group * rest) % LANES
            return pltpu.roll(value, shift, 1) if shift else value

        put_lower(spot, rest_of, lambda side: hshift[layer, kind, side])

    def split_weights(layer):
        pltpu.make_async_copy(w_hbm.at[layer], wbuf.at[layer], load_w.at[layer]).wait()

        def tap(index, carry):
            down, across = index // 3, index % 3
            high, low = split(wbuf[layer, down, across])
            for tile in range(tiles):
                span = slice(tile * LANES, (tile + 1) * LANES)
                base = pl.multiple_of((3 * tile + down) * 3 * LANES, LANES)
                for n, piece in enumerate((high, high, low)):
                    w3[layer, across, pl.ds(base + n * LANES, LANES)] = piece[span]
            return carry

        lax.fori_loop(0, 9, tap, 0)

    def parts_of(sources, seen):
        parts = []
        for row in range(rows):
            downs = [down for down in range(3) if row + down - 1 in sources]
            if downs:
                key = (downs[0], downs[-1] + 1, row in seen)
                if parts and parts[-1][2:] == key and sum(parts[-1][:2]) == row:
                    parts[-1] = (parts[-1][0], parts[-1][1] + 1) + key
                else:
                    parts.append((row, 1) + key)
        seen.update(part[0] + n for part in parts for n in range(part[1]))
        return parts

    def inner(layer, parts, first_tap, taps, which):
        deep = 3 * LANES

        def across(tap, carry):
            for first, count, low, high, add in parts:
                left = jnp.concatenate(
                    [
                        sx[pl.ds(first + down, count), :, pl.ds(tile * deep, deep)].reshape(count * cols, deep)
                        for tile in which
                        for down in range(low, high)
                    ],
                    axis=1,
                )
                right = jnp.concatenate(
                    [
                        w3[layer, tap, pl.ds((3 * tile + low) * deep, (high - low) * deep)]
                        for tile in which
                    ],
                    axis=0,
                )
                total = jnp.dot(left, right, preferred_element_type=jnp.float32)
                total = total.reshape(count, cols, chans)
                if add:
                    acc[layer % 2, tap, pl.ds(first, count), pl.ds(PAD, cols)] += total
                else:
                    acc[layer % 2, tap, pl.ds(first, count), pl.ds(PAD, cols)] = total
            return carry

        lax.fori_loop(first_tap, first_tap + taps, across, 0)

    def outer(layer, kind):
        spot = 0 if kind == FAR else rows + 1
        parts = ((0, 1, 0, 1, True),) if kind == FAR else ((last, 1, 2, 3, True),)
        steps = (both[1:], both[:1]) if layer == layers - 1 and kind == NEAR else (both,)
        for step in steps:

            @pl.when(has_row[kind])
            def _():
                if 1 in step:
                    each_piece(layer, kind, range(2), "wait_recv")
                    put_upper(spot, hmain.at[layer, kind])
                if 0 in step:
                    each_piece(layer, kind, range(2, 5), "wait_recv")
                    put_halo(layer, kind)

            if steps == (both,) or 0 not in step:
                inner(layer, parts, 0, 3, step)

    def finish(layer, row):
        part = acc.at[layer % 2, :, row]
        total = part[0, pl.ds(PAD - 1, cols)] + part[1, pl.ds(PAD, cols)]
        total = jnp.maximum(total + part[2, pl.ds(PAD + 1, cols)], 0.0)
        if layer == layers - 1:
            out[place(row, rows)] = total
        else:
            mid[layer, row] = total

    def blank():
        margin = jnp.zeros((2, 3, rows, PAD, chans), jnp.float32)
        acc[:, :, :, pl.ds(0, PAD)] = margin
        acc[:, :, :, pl.ds(PAD + cols, PAD)] = margin
        for kind, spot in ((FAR, 0), (NEAR, rows + 1)):

            @pl.when(jnp.logical_not(has_row[kind]))
            def _():
                sx[spot] = jnp.zeros((cols, 3 * chans), jnp.bfloat16)

        for side in range(2):

            @pl.when(jnp.logical_not(has_frame[1 - side]))
            def _():
                for layer in range(layers):
                    got[layer, side] = jnp.zeros((rows, part, LANES), jnp.float32)
                    for kind in range(2):
                        hshift[layer, kind, side] = jnp.zeros((part, LANES), jnp.float32)

    pltpu.make_async_copy(x_hbm.at[0], xin, load_x).wait()
    for per_layer in loads_w:
        for load in per_layer:
            load.start()
    pack_half(0, FAR)
    for block in (0, 2, 1):
        pack_frames(0, block)
    pack_half(0, NEAR)
    pl.semaphore_wait(barrier, count)
    send_frames(0, 0)
    send_frames(0, 2)
    for piece in range(3):
        start_far(0, piece)
    send_frames(0, 1)
    start_near(0, False)
    blank()
    for row in range(rows):
        put_row_upper(0, row)
    split_weights(0)
    seen = set()
    parts = parts_of(range(rows), seen)
    inner(0, parts, 0, 1, both[1:])
    start_near(0, True)
    take_frames(0, 0)
    each_piece(0, FAR, range(3, 5), "start")
    take_frames(0, 2)
    each_piece(0, NEAR, range(3, 5), "start")
    inner(0, parts, 1, 1, both[1:])
    forward(0, 0)
    inner(0, parts, 2, 1, both[1:])
    take_frames(0, 1)
    for row in range(rows):
        put_row_lower(0, row)
    parts = parts_of(range(rows), seen)
    forward(0, 1)
    inner(0, parts, 0, 2, both[:1])
    forward(0, 2)
    inner(0, parts, 2, 1, both[:1])
    for layer in range(layers):
        final = layer == layers - 1
        after = layer + 1
        for row in range(1, last):
            finish(layer, row)
        if not final:
            pack_frames(after, 1)
            drain_frames(layer, 1)
            send_frames(after, 1)

            @pl.when(jnp.logical_not(prompt))
            def _():
                split_weights(after)

        outer(layer, FAR)
        finish(layer, 0)
        if not final:
            each_piece(layer, FAR, range(5), "wait_send")
            start_far(after, 0)
            start_far(after, 1)
            pack_half(after, FAR)
            start_far(after, 2)
            pack_frames(after, 0)
            drain_frames(layer, 0)
            send_frames(after, 0)

            @pl.when(prompt)
            def _():
                split_weights(after)

        outer(layer, NEAR)
        if not final:
            finish(layer, last)
            each_piece(layer, NEAR, range(5), "wait_send")
            pack_frames(after, 2)
            drain_frames(layer, 2)
            send_frames(after, 2)
            pack_half(after, NEAR)
            start_near(after, False)
            take_frames(after, 1)
            for row in range(1, last):
                put_row_upper(after, row)
                put_row_lower(after, row)
            seen = set()
            parts = parts_of(range(1, last), seen)
            inner(after, parts, 0, 1, both)
            start_near(after, True)
            inner(after, parts, 1, 1, both)
            for piece in range(3):

                @pl.when(relays(piece))
                def _():
                    relay_copy(layer, piece).wait_send()

            take_frames(after, 0)
            each_piece(after, FAR, range(3, 5), "start")
            forward(after, 0)
            inner(after, parts, 2, 1, both)
            take_frames(after, 2)
            each_piece(after, NEAR, range(3, 5), "start")
            forward(after, 1)
            put_row_upper(after, 0)
            put_row_lower(after, 0)
            inner(after, parts_of((0,), seen), 0, 3, both)
            forward(after, 2)
            put_row_upper(after, last)
            put_row_lower(after, last)
            inner(after, parts_of((last,), seen), 0, 3, both)

    drain(layers - 1)


def store(y_ref, w3, sx, acc, o_hbm, total, ready, sem):
    rows, cols, chans = y_ref.shape
    layers = w3.shape[0]
    last = rows - 1
    deep = 3 * LANES
    turned = lax.axis_index("row") % 2

    def place(row):
        return row + turned * (last - 2 * row)

    copies = [
        pltpu.make_async_copy(y_ref.at[place(row)], o_hbm.at[0, place(row)], sem.at[row]) for row in range(last)
    ]
    for copy in copies:
        copy.start()
    margin = jnp.zeros((3, PAD, chans), jnp.float32)
    total[:, pl.ds(0, PAD)] = margin
    total[:, pl.ds(PAD + cols, PAD)] = margin
    middle = cols // 2
    cuts = ((0, middle + 2 * PAD, 0, middle), (middle + 2 * PAD, cols, middle, cols))
    for n, (start, stop, begin, end) in enumerate(cuts):
        for tap in range(3):
            extra = jnp.dot(
                sx[rows + 1, pl.ds(start, stop - start), pl.ds(0, deep)],
                w3[layers - 1, tap, pl.ds(2 * deep, deep)],
                preferred_element_type=jnp.float32,
            )
            here = pl.ds(PAD + start, stop - start)
            total[tap, here] = acc[(layers - 1) % 2, tap, last, here] + extra
        size = end - begin
        value = total[0, pl.ds(PAD + begin - 1, size)] + total[1, pl.ds(PAD + begin, size)]
        ready[pl.ds(begin, size)] = jnp.maximum(value + total[2, pl.ds(PAD + begin + 1, size)], 0.0)
        copy = pltpu.make_async_copy(
            ready.at[pl.ds(begin, size)], o_hbm.at[0, place(last), pl.ds(begin, size)], sem.at[last + n]
        )
        copy.start()
        copies.append(copy)
    for copy in copies:
        copy.wait()


def local(features, conv_weight):
    _, rows, cols, chans = features.shape
    layers = conv_weight.shape[0]
    fold = chans // 8
    part = cols // (LANES // fold)
    halved = cols // (LANES // (LANES - 2 * fold))
    f32, bf16 = jnp.float32, jnp.bfloat16
    dma = pltpu.SemaphoreType.DMA
    results = pl.pallas_call(
        kernel,
        out_shape=(
            pltpu.VMEM((rows, cols, chans), f32),
            pltpu.VMEM((layers, 3, 9 * chans, chans), bf16),
            pltpu.VMEM((rows + 2, cols, 3 * chans), bf16),
            pltpu.VMEM((2, 3, rows, cols + 2 * PAD, chans), f32),
        ),
        in_specs=[pl.BlockSpec(memory_space=pl.ANY)] * 2,
        out_specs=(pl.BlockSpec(memory_space=pltpu.VMEM),) * 4,
        scratch_shapes=[
            pltpu.VMEM((rows, cols, chans), f32),
            pltpu.VMEM(conv_weight.shape, f32),
            pltpu.VMEM((layers - 1, rows, cols, chans), f32),
            pltpu.VMEM((layers, 2, rows, part, LANES), f32),
            pltpu.VMEM((layers, 2, rows, part, LANES), f32),
            pltpu.VMEM((layers, 2, halved, LANES), f32),
            pltpu.VMEM((layers, 2, cols, chans - LANES), f32),
            pltpu.VMEM((layers, 2, halved, LANES), f32),
            pltpu.VMEM((layers, 2, 2, part, LANES), f32),
            pltpu.VMEM((layers, cols, chans - LANES), f32),
            pltpu.VMEM((layers, halved, LANES), f32),
            dma,
            dma((layers,)),
            dma((2, 5)),
            dma((layers, 2, 5)),
            dma((2, 3)),
            dma((layers, 2, 3)),
            dma((3,)),
            dma((layers, 3)),
        ],
        compiler_params=pltpu.CompilerParams(
            collective_id=0, has_side_effects=True, vmem_limit_bytes=47 * 1024 * 1024
        ),
    )(features, conv_weight)
    return pl.pallas_call(
        store,
        out_shape=jax.ShapeDtypeStruct(features.shape, f32),
        in_specs=[pl.BlockSpec(memory_space=pltpu.VMEM)] * 4,
        out_specs=pl.BlockSpec(memory_space=pl.ANY),
        scratch_shapes=[
            pltpu.VMEM((3, cols + 2 * PAD, chans), f32),
            pltpu.VMEM((cols, chans), f32),
            dma((rows + 1,)),
        ],
        compiler_params=pltpu.CompilerParams(vmem_limit_bytes=4 * 1024 * 1024),
    )(*results)


def solution(mesh):
    placed = (P("frame", "row", None, None), P())
    return jax.shard_map(
        local, mesh=mesh, in_specs=placed, out_specs=P("frame", "row", None, None), check_vma=False
    )
```

```python
import jax
import jax.numpy as jnp
from jax import lax
from jax.experimental import pallas as pl
from jax.experimental.pallas import tpu as pltpu
from jax.sharding import PartitionSpec as P

MESH = pl.DeviceIdType.MESH
LANES = 128
PAD = 8
FAR, NEAR = 0, 1


def split(value):
    high = value.astype(jnp.bfloat16)
    low = (value - high.astype(jnp.float32)).astype(jnp.bfloat16)
    return high, low


def kernel(
    x_hbm, w_hbm, out, w3, sx, acc, xin, wbuf, mid, pack, got, half, hmain, hhalf, hshift, rmain, rhalf,
    load_x, load_w, row_send, row_recv, frame_send, frame_recv, relay_send, relay_recv,
):
    rows, cols, chans = xin.shape
    layers = wbuf.shape[0]
    tiles = chans // LANES
    both = range(tiles)
    fold = chans // 8
    last = rows - 1
    groups = LANES // fold
    part = cols // groups
    rest = LANES - 2 * fold
    halves = LANES // rest
    frames, bands = lax.axis_size("frame"), lax.axis_size("row")
    t, r = lax.axis_index("frame"), lax.axis_index("row")
    turned = r % 2
    sign = 1 - 2 * turned
    row_to = (r - sign, r + sign)
    has_row = tuple((peer >= 0) & (peer < bands) for peer in row_to)
    edge = (0, last)
    has_frame = (t > 0, t < frames - 1)
    frame_to = (t - 1, t + 1)

    pairs = bands // 2

    def shared(place):
        step = place // 2
        return 4 * (step + (place % 2) * (pairs - 1 - 2 * step)) // pairs

    def takes(place, piece):
        return shared(place) > piece

    def within(place):
        return (place >= 0) & (place < bands)

    def relayed(piece):
        return has_row[FAR] & has_row[NEAR] & takes(r, piece)

    onward = r + 2 * sign
    behind = r - 2 * sign

    def relays(piece):
        return has_row[NEAR] & within(onward) & takes(row_to[NEAR], piece)

    def place(row, count):
        return row + turned * (count - 1 - 2 * row)

    loads_x = [pltpu.make_async_copy(x_hbm.at[0, place(q, rows)], xin.at[q], load_x) for q in range(rows)]
    loads_w = [
        [pltpu.make_async_copy(w_hbm.at[n, place(d, 3)], wbuf.at[n, d], load_w.at[n]) for d in range(3)]
        for n in range(layers)
    ]
    for load in loads_x:
        load.start()

    barrier = pltpu.get_barrier_semaphore()
    count = 0
    for have, axis, peers in ((has_row, "row", row_to), (has_frame, "frame", frame_to)):
        for side in range(2):
            count = count + have[side].astype(jnp.int32)

            @pl.when(have[side])
            def _():
                pl.semaphore_signal(barrier, inc=1, device_id={axis: peers[side]}, device_id_type=MESH)

    for peer in (onward, behind):
        count = count + within(peer).astype(jnp.int32)

        @pl.when(within(peer))
        def _():
            pl.semaphore_signal(barrier, inc=1, device_id={"row": peer}, device_id_type=MESH)

    def maps(layer):
        return xin if layer == 0 else mid.at[layer - 1]

    def section(piece):
        return pl.ds(piece * (cols // 2), cols // 2)

    def row_copy(layer, kind, piece, relay=False):
        if piece < 2:
            source = maps(layer).at[edge[kind], section(piece), pl.ds(LANES, chans - LANES)]
            target = (rmain.at[layer] if relay else hmain.at[layer, kind]).at[section(piece)]
        elif piece == 2:
            source = half.at[layer, kind]
            target = rhalf.at[layer] if relay else hhalf.at[layer, kind]
        else:
            source = got.at[layer, piece - 3, edge[kind]]
            target = hshift.at[layer, kind, piece - 3]
        return pltpu.make_async_remote_copy(
            src_ref=source,
            dst_ref=target,
            send_sem=row_send.at[kind, piece],
            recv_sem=relay_recv.at[layer, piece] if relay else row_recv.at[layer, kind, piece],
            device_id={"row": row_to[NEAR if relay else kind]},
            device_id_type=MESH,
        )

    def relay_copy(layer, piece):
        if piece < 2:
            source, target = (ref.at[section(piece)] for ref in (rmain.at[layer], hmain.at[layer, FAR]))
        else:
            source, target = rhalf.at[layer], hhalf.at[layer, FAR]
        return pltpu.make_async_remote_copy(
            src_ref=source,
            dst_ref=target,
            send_sem=relay_send.at[piece],
            recv_sem=row_recv.at[layer, FAR, piece],
            device_id={"row": onward},
            device_id_type=MESH,
        )

    def start_far(layer, piece):
        @pl.when(relayed(piece))
        def _():
            row_copy(layer, FAR, piece, True).start()

        @pl.when(has_row[FAR] & jnp.logical_not(relayed(piece)))
        def _():
            row_copy(layer, FAR, piece).start()

    def drain_frames(layer, block):
        for side in range(2):

            @pl.when(has_frame[side])
            def _():
                frame_copy(layer, side, block).wait_send()

    def drain(layer):
        for kind in range(2):
            each_piece(layer, kind, range(5), "wait_send")
        for piece in range(3):

            @pl.when(relays(piece))
            def _():
                relay_copy(layer, piece).wait_send()

        for block in range(len(blocks)):
            drain_frames(layer, block)

    def start_near(layer, late):
        @pl.when(has_row[NEAR] & (relayed(1) if late else jnp.logical_not(relayed(1))))
        def _():
            for piece in range(3):
                row_copy(layer, NEAR, piece).start()

    def forward(layer, piece):
        @pl.when(relays(piece))
        def _():
            row_copy(layer, FAR, piece, True).wait_recv()
            relay_copy(layer, piece).start()

    def sent(kind, piece):
        return has_row[kind] if piece < 3 else has_row[kind] & has_frame[4 - piece]

    prompt = has_row[FAR] & (shared(row_to[FAR]) <= 1)

    def each_piece(layer, kind, pieces, action):
        for piece in pieces:

            @pl.when(sent(kind, piece))
            def _():
                getattr(row_copy(layer, kind, piece), action)()

    blocks = ((0, 1), (1, rows - 2), (last, 1))

    def frame_copy(layer, side, block):
        start, size = blocks[block]
        return pltpu.make_async_remote_copy(
            src_ref=pack.at[layer, side, pl.ds(start, size)],
            dst_ref=got.at[layer, side, pl.ds(start, size)],
            send_sem=frame_send.at[side, block],
            recv_sem=frame_recv.at[layer, side, block],
            device_id={"frame": frame_to[side]},
            device_id_type=MESH,
        )

    def pack_frames(layer, block):
        start, size = blocks[block]
        lane = lax.broadcasted_iota(jnp.int32, (part, LANES), 1)
        for side in range(2):
            for row in range(start, start + size):
                full = None
                for group in range(groups):
                    value = maps(layer)[row, pl.ds(group * part, part), pl.ds(0, LANES)]
                    shift = ((group - side) * fold) % LANES
                    value = pltpu.roll(value, shift, 1) if shift else value
                    full = value if full is None else jnp.where(lane // fold == group, value, full)
                pack[layer, side, row] = full

    def send_frames(layer, block):
        for side in range(2):

            @pl.when(has_frame[side])
            def _():
                frame_copy(layer, side, block).start()

    def take_frames(layer, block):
        for side in range(2):

            @pl.when(has_frame[1 - side])
            def _():
                frame_copy(layer, side, block).wait_recv()

    def pack_half(layer, kind):
        size = cols // halves
        lane = lax.broadcasted_iota(jnp.int32, (size, LANES), 1)
        full = None
        for group in range(halves):
            value = maps(layer)[edge[kind], pl.ds(group * size, size), pl.ds(0, LANES)]
            shift = (group * rest - 2 * fold) % LANES
            value = pltpu.roll(value, shift, 1) if shift else value
            full = value if full is None else jnp.where(lane // rest == group, value, full)
        half[layer, kind] = full

    def put(spot, start, size, tile, value):
        high, low = split(value)
        for n, piece in enumerate((high, low, high)):
            sx[spot, pl.ds(start, size), pl.ds((3 * tile + n) * LANES, LANES)] = piece

    def put_upper(spot, source):
        for tile in range(1, tiles):
            put(spot, 0, cols, tile, source[:, pl.ds((tile - 1) * LANES, LANES)])

    def put_lower(spot, rest_of, shifted):
        lane = lax.broadcasted_iota(jnp.int32, (part, LANES), 1)
        for group in range(groups):
            value = rest_of(group * part)
            for side in range(2):
                moved = shifted(side)
                shift = ((side - group) * fold) % LANES
                moved = pltpu.roll(moved, shift, 1) if shift else moved
                value = jnp.where(lane // fold == side, moved, value)
            put(spot, group * part, part, 0, value)

    def put_row_upper(layer, row):
        put_upper(row + 1, maps(layer).at[row, :, pl.ds(LANES, chans - LANES)])

    def put_row_lower(layer, row):
        put_lower(
            row + 1,
            lambda start: maps(layer)[row, pl.ds(start, part), pl.ds(0, LANES)],
            lambda side: got[layer, side, row],
        )

    def put_halo(layer, kind):
        spot = 0 if kind == FAR else rows + 1
        size = cols // halves

        def rest_of(start):
            group = start // size
            value = hhalf[layer, kind, pl.ds(start - group * size, part)]
            shift = (2 * fold - group * rest) % LANES
            return pltpu.roll(value, shift, 1) if shift else value

        put_lower(spot, rest_of, lambda side: hshift[layer, kind, side])

    def split_weights(layer):
        pltpu.make_async_copy(w_hbm.at[layer], wbuf.at[layer], load_w.at[layer]).wait()

        def tap(index, carry):
            down, across = index // 3, index % 3
            high, low = split(wbuf[layer, down, across])
            for tile in range(tiles):
                span = slice(tile * LANES, (tile + 1) * LANES)
                base = pl.multiple_of((3 * tile + down) * 3 * LANES, LANES)
                for n, piece in enumerate((high, high, low)):
                    w3[layer, across, pl.ds(base + n * LANES, LANES)] = piece[span]
            return carry

        lax.fori_loop(0, 9, tap, 0)

    def parts_of(sources, seen):
        parts = []
        for row in range(rows):
            downs = [down for down in range(3) if row + down - 1 in sources]
            if downs:
                key = (downs[0], downs[-1] + 1, row in seen)
                if parts and parts[-1][2:] == key and sum(parts[-1][:2]) == row:
                    parts[-1] = (parts[-1][0], parts[-1][1] + 1) + key
                else:
                    parts.append((row, 1) + key)
        seen.update(part[0] + n for part in parts for n in range(part[1]))
        return parts

    def inner(layer, parts, first_tap, taps, which):
        deep = 3 * LANES

        def across(tap, carry):
            for first, count, low, high, add in parts:
                left = jnp.concatenate(
                    [
                        sx[pl.ds(first + down, count), :, pl.ds(tile * deep, deep)].reshape(count * cols, deep)
                        for tile in which
                        for down in range(low, high)
                    ],
                    axis=1,
                )
                right = jnp.concatenate(
                    [
                        w3[layer, tap, pl.ds((3 * tile + low) * deep, (high - low) * deep)]
                        for tile in which
                    ],
                    axis=0,
                )
                total = jnp.dot(left, right, preferred_element_type=jnp.float32)
                total = total.reshape(count, cols, chans)
                if add:
                    acc[layer % 2, tap, pl.ds(first, count), pl.ds(PAD, cols)] += total
                else:
                    acc[layer % 2, tap, pl.ds(first, count), pl.ds(PAD, cols)] = total
            return carry

        lax.fori_loop(first_tap, first_tap + taps, across, 0)

    def outer(layer, kind):
        spot = 0 if kind == FAR else rows + 1
        parts = ((0, 1, 0, 1, True),) if kind == FAR else ((last, 1, 2, 3, True),)
        steps = (both[1:], both[:1]) if layer == layers - 1 and kind == NEAR else (both,)
        for step in steps:

            @pl.when(has_row[kind])
            def _():
                if 1 in step:
                    each_piece(layer, kind, range(2), "wait_recv")
                    put_upper(spot, hmain.at[layer, kind])
                if 0 in step:
                    each_piece(layer, kind, range(2, 5), "wait_recv")
                    put_halo(layer, kind)

            if steps == (both,) or 0 not in step:
                inner(layer, parts, 0, 3, step)

    def finish(layer, row):
        part = acc.at[layer % 2, :, row]
        total = part[0, pl.ds(PAD - 1, cols)] + part[1, pl.ds(PAD, cols)]
        total = jnp.maximum(total + part[2, pl.ds(PAD + 1, cols)], 0.0)
        if layer == layers - 1:
            out[place(row, rows)] = total
        else:
            mid[layer, row] = total

    def blank():
        margin = jnp.zeros((2, 3, rows, PAD, chans), jnp.float32)
        acc[:, :, :, pl.ds(0, PAD)] = margin
        acc[:, :, :, pl.ds(PAD + cols, PAD)] = margin
        for kind, spot in ((FAR, 0), (NEAR, rows + 1)):

            @pl.when(jnp.logical_not(has_row[kind]))
            def _():
                sx[spot] = jnp.zeros((cols, 3 * chans), jnp.bfloat16)

        for side in range(2):

            @pl.when(jnp.logical_not(has_frame[1 - side]))
            def _():
                for layer in range(layers):
                    got[layer, side] = jnp.zeros((rows, part, LANES), jnp.float32)
                    for kind in range(2):
                        hshift[layer, kind, side] = jnp.zeros((part, LANES), jnp.float32)

    pltpu.make_async_copy(x_hbm.at[0], xin, load_x).wait()
    for per_layer in loads_w:
        for load in per_layer:
            load.start()
    pack_half(0, FAR)
    for block in (0, 2, 1):
        pack_frames(0, block)
    pack_half(0, NEAR)
    pl.semaphore_wait(barrier, count)
    send_frames(0, 0)
    send_frames(0, 2)
    for piece in range(3):
        start_far(0, piece)
    send_frames(0, 1)
    start_near(0, False)
    blank()
    for row in range(rows):
        put_row_upper(0, row)
    split_weights(0)
    seen = set()
    parts = parts_of(range(rows), seen)
    inner(0, parts, 0, 1, both[1:])
    start_near(0, True)
    take_frames(0, 0)
    each_piece(0, FAR, range(3, 5), "start")
    take_frames(0, 2)
    each_piece(0, NEAR, range(3, 5), "start")
    inner(0, parts, 1, 1, both[1:])
    forward(0, 0)
    inner(0, parts, 2, 1, both[1:])
    take_frames(0, 1)
    for row in range(rows):
        put_row_lower(0, row)
    parts = parts_of(range(rows), seen)
    forward(0, 1)
    inner(0, parts, 0, 2, both[:1])
    forward(0, 2)
    inner(0, parts, 2, 1, both[:1])
    for layer in range(layers):
        final = layer == layers - 1
        after = layer + 1
        for row in range(1, last):
            finish(layer, row)
        if not final:
            pack_frames(after, 1)
            drain_frames(layer, 1)
            send_frames(after, 1)

            @pl.when(jnp.logical_not(prompt))
            def _():
                split_weights(after)

        outer(layer, FAR)
        finish(layer, 0)
        if not final:
            each_piece(layer, FAR, range(5), "wait_send")
            start_far(after, 0)
            start_far(after, 1)
            pack_half(after, FAR)
            start_far(after, 2)
            pack_frames(after, 0)
            drain_frames(layer, 0)
            send_frames(after, 0)

            @pl.when(prompt)
            def _():
                split_weights(after)

        outer(layer, NEAR)
        if not final:
            finish(layer, last)
            each_piece(layer, NEAR, range(5), "wait_send")
            pack_frames(after, 2)
            drain_frames(layer, 2)
            send_frames(after, 2)
            pack_half(after, NEAR)
            start_near(after, False)
            take_frames(after, 1)
            for row in range(1, last):
                put_row_upper(after, row)
                put_row_lower(after, row)
            seen = set()
            parts = parts_of(range(1, last), seen)
            inner(after, parts, 0, 1, both)
            start_near(after, True)
            for piece in range(3):

                @pl.when(relays(piece))
                def _():
                    relay_copy(layer, piece).wait_send()

            take_frames(after, 0)
            each_piece(after, FAR, range(3, 5), "start")
            forward(after, 0)
            inner(after, parts, 1, 2, both)
            take_frames(after, 2)
            each_piece(after, NEAR, range(3, 5), "start")
            forward(after, 1)
            put_row_upper(after, 0)
            put_row_lower(after, 0)
            inner(after, parts_of((0,), seen), 0, 3, both)
            forward(after, 2)
            put_row_upper(after, last)
            put_row_lower(after, last)
            inner(after, parts_of((last,), seen), 0, 3, both)

    drain(layers - 1)


def store(y_ref, w3, sx, acc, o_hbm, total, ready, sem):
    rows, cols, chans = y_ref.shape
    layers = w3.shape[0]
    last = rows - 1
    deep = 3 * LANES
    turned = lax.axis_index("row") % 2

    def place(row):
        return row + turned * (last - 2 * row)

    copies = [
        pltpu.make_async_copy(y_ref.at[place(row)], o_hbm.at[0, place(row)], sem.at[row]) for row in range(last)
    ]
    for copy in copies:
        copy.start()
    margin = jnp.zeros((3, PAD, chans), jnp.float32)
    total[:, pl.ds(0, PAD)] = margin
    total[:, pl.ds(PAD + cols, PAD)] = margin
    middle = cols // 2
    cuts = ((0, middle + 2 * PAD, 0, middle), (middle + 2 * PAD, cols, middle, cols))
    for n, (start, stop, begin, end) in enumerate(cuts):
        for tap in range(3):
            extra = jnp.dot(
                sx[rows + 1, pl.ds(start, stop - start), pl.ds(0, deep)],
                w3[layers - 1, tap, pl.ds(2 * deep, deep)],
                preferred_element_type=jnp.float32,
            )
            here = pl.ds(PAD + start, stop - start)
            total[tap, here] = acc[(layers - 1) % 2, tap, last, here] + extra
        size = end - begin
        value = total[0, pl.ds(PAD + begin - 1, size)] + total[1, pl.ds(PAD + begin, size)]
        ready[pl.ds(begin, size)] = jnp.maximum(value + total[2, pl.ds(PAD + begin + 1, size)], 0.0)
        copy = pltpu.make_async_copy(
            ready.at[pl.ds(begin, size)], o_hbm.at[0, place(last), pl.ds(begin, size)], sem.at[last + n]
        )
        copy.start()
        copies.append(copy)
    for copy in copies:
        copy.wait()


def local(features, conv_weight):
    _, rows, cols, chans = features.shape
    layers = conv_weight.shape[0]
    fold = chans // 8
    part = cols // (LANES // fold)
    halved = cols // (LANES // (LANES - 2 * fold))
    f32, bf16 = jnp.float32, jnp.bfloat16
    dma = pltpu.SemaphoreType.DMA
    results = pl.pallas_call(
        kernel,
        out_shape=(
            pltpu.VMEM((rows, cols, chans), f32),
            pltpu.VMEM((layers, 3, 9 * chans, chans), bf16),
            pltpu.VMEM((rows + 2, cols, 3 * chans), bf16),
            pltpu.VMEM((2, 3, rows, cols + 2 * PAD, chans), f32),
        ),
        in_specs=[pl.BlockSpec(memory_space=pl.ANY)] * 2,
        out_specs=(pl.BlockSpec(memory_space=pltpu.VMEM),) * 4,
        scratch_shapes=[
            pltpu.VMEM((rows, cols, chans), f32),
            pltpu.VMEM(conv_weight.shape, f32),
            pltpu.VMEM((layers - 1, rows, cols, chans), f32),
            pltpu.VMEM((layers, 2, rows, part, LANES), f32),
            pltpu.VMEM((layers, 2, rows, part, LANES), f32),
            pltpu.VMEM((layers, 2, halved, LANES), f32),
            pltpu.VMEM((layers, 2, cols, chans - LANES), f32),
            pltpu.VMEM((layers, 2, halved, LANES), f32),
            pltpu.VMEM((layers, 2, 2, part, LANES), f32),
            pltpu.VMEM((layers, cols, chans - LANES), f32),
            pltpu.VMEM((layers, halved, LANES), f32),
            dma,
            dma((layers,)),
            dma((2, 5)),
            dma((layers, 2, 5)),
            dma((2, 3)),
            dma((layers, 2, 3)),
            dma((3,)),
            dma((layers, 3)),
        ],
        compiler_params=pltpu.CompilerParams(
            collective_id=0, has_side_effects=True, vmem_limit_bytes=47 * 1024 * 1024
        ),
    )(features, conv_weight)
    return pl.pallas_call(
        store,
        out_shape=jax.ShapeDtypeStruct(features.shape, f32),
        in_specs=[pl.BlockSpec(memory_space=pltpu.VMEM)] * 4,
        out_specs=pl.BlockSpec(memory_space=pl.ANY),
        scratch_shapes=[
            pltpu.VMEM((3, cols + 2 * PAD, chans), f32),
            pltpu.VMEM((cols, chans), f32),
            dma((rows + 1,)),
        ],
        compiler_params=pltpu.CompilerParams(vmem_limit_bytes=4 * 1024 * 1024),
    )(*results)


def solution(mesh):
    placed = (P("frame", "row", None, None), P())
    return jax.shard_map(
        local, mesh=mesh, in_specs=placed, out_specs=P("frame", "row", None, None), check_vma=False
    )
```
